128 devices in a mesh: row: 8 (over z_hi, y), col: 16 (over x, z_lo, core).
Axes of the slice: x: 4, y: 4, z: 4 (z_hi: 2, z_lo: 2; z = z_hi * 2 + z_lo), core: 2. Of those that a mesh axis runs over, the one named last changes fastest.
Arguments:
- student_hidden: bfloat16 [16384, 1920], P(('row', 'col')), may hold values from -6 to 6
- projection: bfloat16 [1920, 768], replicated, may hold values from -0.125 to 0.125
- teacher: bfloat16 [10240, 768], P(('row', 'col')), may hold values from -6 to 6
- block_map: int32 [128, 3, 4096], P(('row', 'col')), may hold values from 0 to 127, as said below
- block_counts: int32 [128, 128], P(('row', 'col')), may hold values from 16 to 32, as said below
- interp_weights: float32 [64], replicated, may hold values from 0.1 to 1
Outputs:
- grad_hidden: bfloat16 [16384, 1920], P(('row', 'col'))
The draws below stay inside these ranges and needn't reach their ends.
Inputs may be any that keep to these rules, and one draw needn't show every extreme that they name: `block_map`: field 0 is a tubelet of the sending device below 80, field 1 a cell of the receiving device below 128, field 2 a level below 64. Slots to the sending device itself name cells near the tubelet's proportional position; slots to other devices name any of their cells. Dead slots hold values in range. `block_counts`: entry [s, d] counts the live slots from device s to device d, at the start of d's 32 slots; it is at least 16. In every draw some device receives 32 blocks from every device.
All inputs are finite; a program needn't handle non-finite values.
Results may differ from the reference program's by a relative error of at most 0.025.
Values may be sent and summed in bfloat16 or wider, within the bound.
A program may use at most 64 MiB of HBM per device.

```python
import jax
import jax.numpy as jnp
from jax import lax

D_HID = 1920
D_REP = 768
TOK_DEV = 128
TUB_DEV = 80
CAP = 32
LEVELS = 64
TOKENS = 16384
TUBES = 10240
N_ROW = 8
DEVICES = 128


def draw_block_map(key, part):
    first, second, third, fifth = jax.random.split(jax.random.fold_in(key, 11), 4)
    shape = (DEVICES, DEVICES * CAP)
    sender = jnp.arange(DEVICES, dtype=jnp.int32)[:, None]
    receiver = (jnp.arange(DEVICES * CAP, dtype=jnp.int32) // CAP)[None, :]
    offset = receiver - sender
    tubes = jax.random.randint(first, shape, 0, TUB_DEV)
    jitter = max(TOK_DEV // 8, 1)
    centre = tubes * TOK_DEV // TUB_DEV + jax.random.randint(second, shape, -jitter, jitter + 1)
    centre = jnp.clip(centre, 0, TOK_DEV - 1)
    spread = jax.random.randint(third, shape, 0, TOK_DEV)
    cells = jnp.where(offset == 0, centre, spread)
    levels = jax.random.randint(fifth, shape, 0, LEVELS)
    return jnp.stack([tubes, cells, levels], axis=1).astype(jnp.int32)


def draw_block_counts(key, part):
    first, second = jax.random.split(jax.random.fold_in(key, 23))
    base = jax.random.randint(first, (DEVICES, DEVICES), CAP // 2, CAP + 1)
    busiest = jax.random.randint(second, (), 0, DEVICES)
    column = jnp.arange(DEVICES, dtype=jnp.int32)[None, :]
    counts = jnp.where(column == busiest, CAP, base)
    return counts.astype(jnp.int32)


def steps_of(own_key, dims, shards, least, top_value):
    level, own = 1.0, jax.random.fold_in(own_key, 6)
    for position, parts in shards:
        steps = jnp.exp(jax.random.uniform(jax.random.fold_in(own, position), (parts,), jnp.float32, least / len(shards), top_value / len(shards)))
        level = level * jnp.repeat(steps, dims[position] // parts).reshape([-1 if axis == position else 1 for axis in range(len(dims))])
    return level


def normal_values(stream_key, shape, scale, most, shards=(), kind=jnp.bfloat16):
    entries = scale * jax.random.normal(stream_key, shape, jnp.float32)
    if shards:
        entries = entries * steps_of(stream_key, shape, shards, -0.22, 0.18)
    return jnp.clip(entries, -most, most).astype(kind)


def setup_inputs(seed: int = 0) -> dict:
    streams_of = jax.random.split(jax.random.key(seed), 7)
    student_hidden = normal_values(streams_of[0], (TOKENS, D_HID), 1.0, 6.0, ((0, 128),))
    projection = normal_values(streams_of[1], (D_HID, D_REP), D_HID ** -0.5, 0.125)
    teacher = normal_values(streams_of[2], (TUBES, D_REP), 1.0, 6.0, ((0, 128),))
    block_map = draw_block_map(jax.random.fold_in(streams_of[6], 71), 0)
    block_counts = draw_block_counts(jax.random.fold_in(streams_of[6], 71), 0)
    interp_weights = jnp.clip(jax.random.uniform(streams_of[5], (LEVELS,), jnp.float32, 0.1, 1.0), 0.1, 1.0)
    return {"student_hidden": student_hidden, "projection": projection, "teacher": teacher, "block_map": block_map, "block_counts": block_counts, "interp_weights": interp_weights}


huber_delta = 0.05
norm_eps = 1e-06

def reference(student_hidden, projection, teacher, block_map, block_counts, interp_weights):
    devices = block_map.shape[0]
    slots = block_map.shape[2]
    per_peer = slots // devices
    tokens_dev = student_hidden.shape[0] // devices
    tubes_dev = teacher.shape[0] // devices
    width = teacher.shape[1]
    levels = interp_weights[block_map[:, 2, :]]
    live = (jnp.arange(per_peer, dtype=jnp.int32)[None, None, :] < block_counts[:, :, None]).reshape(devices, slots)
    scales = levels * live.astype(jnp.float32)
    tube_global = (block_map[:, 0, :] + (jnp.arange(devices, dtype=jnp.int32) * tubes_dev)[:, None]).astype(jnp.int32)
    cell_local = block_map[:, 1, :]

    def target_of(dest):
        start = (dest * per_peer).astype(jnp.int32)
        tubes = lax.dynamic_slice_in_dim(tube_global, start, per_peer, 1).reshape(-1)
        scale = lax.dynamic_slice_in_dim(scales, start, per_peer, 1).reshape(-1)
        cells = lax.dynamic_slice_in_dim(cell_local, start, per_peer, 1).reshape(-1)
        rows = teacher[tubes]
        contrib = (rows.astype(jnp.float32) * scale[:, None]).astype(jnp.bfloat16)
        onehot = (cells[None, :] == jnp.arange(tokens_dev, dtype=jnp.int32)[:, None]).astype(jnp.bfloat16)
        return jnp.dot(onehot, contrib, preferred_element_type=jnp.float32)
    target = lax.map(target_of, jnp.arange(devices, dtype=jnp.int32)).reshape(devices * tokens_dev, width)
    teacher_unit = (target * lax.rsqrt(lax.optimization_barrier(jnp.sum(target * target, axis=1, keepdims=True)) + norm_eps)).astype(jnp.bfloat16)
    proj = jnp.dot(student_hidden, projection, preferred_element_type=jnp.float32)
    inverse = lax.rsqrt(lax.optimization_barrier(jnp.sum(proj * proj, axis=1, keepdims=True)) + norm_eps)
    unit = proj * inverse
    student_unit = unit.astype(jnp.bfloat16)
    total = student_unit.shape[0]
    strip_rows = total // N_ROW
    contract = (((1,), (1,)), ((), ()))

    def strip(start):
        block_s = lax.dynamic_slice_in_dim(student_unit, start, strip_rows, 0)
        block_t = lax.dynamic_slice_in_dim(teacher_unit, start, strip_rows, 0)
        gram_s = lax.dot_general(block_s, student_unit, contract, preferred_element_type=jnp.float32)
        gram_t = lax.dot_general(block_t, teacher_unit, contract, preferred_element_type=jnp.float32)
        slope = jnp.clip((gram_s - gram_t) / huber_delta, -1.0, 1.0).astype(jnp.bfloat16)
        return 2.0 * jnp.dot(slope, student_unit, preferred_element_type=jnp.float32)
    starts = jnp.arange(N_ROW, dtype=jnp.int32) * strip_rows
    grad_unit = lax.map(strip, starts).reshape(total, width)
    along = lax.optimization_barrier(jnp.sum(unit * grad_unit, axis=1, keepdims=True))
    grad_proj = ((grad_unit - unit * along) * inverse).astype(jnp.bfloat16)
    grad_hidden = lax.dot_general(grad_proj, projection, contract, preferred_element_type=jnp.float32)
    return grad_hidden.astype(jnp.bfloat16)
```

```python
import functools

import jax
import jax.numpy as jnp
from jax import lax
from jax.experimental import pallas as pl
from jax.experimental.pallas import tpu as pltpu
from jax.sharding import PartitionSpec as P

BOTH = ("row", "col")
MESH = pl.DeviceIdType.MESH
NT = (((1,), (1,)), ((), ()))

huber_delta = 0.05
norm_eps = 1e-06


class Place:
    def __init__(self):
        row, col = lax.axis_index("row"), lax.axis_index("col")
        self.zh, self.y = row // 4, row % 4
        self.x, self.zl, self.core = col // 4, (col // 2) % 2, col % 2

    def row_of(self, d, q):
        return (self.zh + q) % 2 * 4 + (self.y + d) % 4

    def a(self, d, q, k=0):
        col = (self.x + d) % 4 * 4 + (self.zl + q) % 2 * 2 + (self.core + k) % 2
        return (self.zh * 4 + self.y, col)

    def b(self, d, q):
        col = self.x * 4 + (self.zl + q) % 2 * 2 + self.core
        return (self.row_of(d, q), col)


def greet(peers):
    barrier = pltpu.get_barrier_semaphore()
    for peer in peers:
        pl.semaphore_signal(barrier, inc=1, device_id=peer, device_id_type=MESH)
    pl.semaphore_wait(barrier, len(peers))


def remote(src, dst, send, recv, i, device):
    return pltpu.make_async_remote_copy(
        src_ref=src,
        dst_ref=dst,
        send_sem=send.at[i],
        recv_sem=recv.at[i],
        device_id=device,
        device_id_type=MESH,
    )


def gather(own, buf, send, recv, to, cut, twin=None):
    rest = own.shape[0] - cut
    lo, hi = pl.ds(0, cut), pl.ds(cut, rest)
    ahead, behind, across = to(1, 0), to(3, 0), to(0, 1)
    plan = [
        (own, buf.at[3], ahead),
        (own, buf.at[1], behind),
        (own, buf.at[4], across),
        (buf.at[3, lo], buf.at[2, lo], ahead),
        (buf.at[1, hi], buf.at[2, hi], behind),
        (buf.at[4], buf.at[7], ahead),
        (buf.at[4], buf.at[5], behind),
        (buf.at[2, lo], buf.at[6, lo], across),
        (buf.at[2, hi], buf.at[6, hi], across),
    ]
    copies = [remote(s, d, send, recv, i, dev) for i, (s, d, dev) in enumerate(plan)]
    twins = []

    def pass_on(src, slot):
        if twin is not None:
            copy = remote(src, buf.at[8 + slot], send, recv, 9 + slot, twin)
            copy.start()
            twins.append(copy)

    for i in (0, 1, 2):
        copies[i].start()
    pass_on(own, 0)
    buf[0] = own[...]
    yield
    after = ((0, (3,), 3), (1, (4,), 1), (2, (5, 6), 4), (3, (7,), None), (4, (8,), 2))
    after += ((5, (), 7), (6, (), 5), (7, (), None), (8, (), 6))
    for i, starts, slot in after:
        copies[i].wait_recv()
        for j in starts:
            copies[j].start()
        if slot is not None:
            pass_on(buf.at[slot], slot)
        yield
    for copy in twins:
        copy.wait_recv()
    for copy in copies + twins:
        copy.wait_send()


def together(*plans):
    plans = list(plans)
    while plans:
        for plan in list(plans):
            try:
                next(plan)
            except StopIteration:
                plans.remove(plan)


def scatter(blocks, block_of, buf, send, recv, to):
    copies = []
    for q in (0, 1):
        for d in (1, 3, 2, 0):
            if q or d:
                slot = q * 4 + (4 - d) % 4
                src = blocks.at[block_of(d, q)]
                copies.append(remote(src, buf.at[slot], send, recv, slot, to(d, q)))
                copies[-1].start()
    buf[0] = blocks[block_of(0, 0)]
    yield
    for copy in copies:
        copy.wait_recv()
    for copy in copies:
        copy.wait_send()


def a_near(me):
    return [me.a(1, 0), me.a(3, 0), me.a(0, 1), me.a(0, 0, 1)]


def b_near(me):
    return [me.b(1, 0), me.b(3, 0), me.b(0, 1)]


def first_kernel(teacher, own, notes, teachers, column, told, s1, r1, s2, r2, s3, r3):
    me = Place()
    others = [(d, q, k) for k in (0, 1) for q in (0, 1) for d in range(4) if d or q or k]
    greet([me.a(*o) for o in others] + b_near(me))
    copies = []
    for d, q, k in others:
        twist = (me.zh + me.zl + q) % 2
        note = (me.x + d) % 4 * 4 + twist * 2 + (me.core + k) % 2
        slot = k * 8 + q * 4 + (4 - d) % 4
        copies.append(remote(notes.at[note], told.at[slot], s3, r3, slot, me.a(d, q, k)))
        copies[-1].start()
    told[0] = notes[me.x * 4 + (me.zh + me.zl) % 2 * 2 + me.core]
    together(
        gather(teacher, teachers, s1, r1, me.a, 48, me.a(0, 0, 1)),
        gather(own, column, s2, r2, me.b, 64),
    )
    for copy in copies:
        copy.wait_recv()
    for copy in copies:
        copy.wait_send()


def second_kernel(own, parts, line, arrived, s1, r1, s2, r2):
    me = Place()
    far = [me.b(d, q) for q in (0, 1) for d in range(4) if d or q]
    greet(a_near(me) + far)
    together(
        scatter(parts, me.row_of, arrived, s2, r2, me.b),
        gather(own, line, s1, r1, me.a, 64, me.a(0, 0, 1)),
    )


def third_kernel(own, line, column, s1, r1, s2, r2):
    me = Place()
    greet(a_near(me) + b_near(me))
    together(
        gather(own, line, s1, r1, me.a, 64, me.a(0, 0, 1)),
        gather(own, column, s2, r2, me.b, 64),
    )


def fourth_kernel(parts, arrived, s1, r1):
    me = Place()
    greet([me.b(d, q) for q in (0, 1) for d in range(4) if d or q])
    together(scatter(parts, lambda d, q: q * 4 + d, arrived, s1, r1, me.b))


def exchange(kernel, number, outs, sems, *args):
    return pl.pallas_call(
        kernel,
        out_shape=[jax.ShapeDtypeStruct(s, t) for s, t in outs],
        in_specs=[pl.BlockSpec(memory_space=pltpu.VMEM)] * len(args),
        out_specs=[pl.BlockSpec(memory_space=pltpu.VMEM)] * len(outs),
        scratch_shapes=[pltpu.SemaphoreType.DMA((n,)) for n in sems for _ in (0, 1)],
        compiler_params=pltpu.CompilerParams(
            collective_id=number, has_side_effects=True, vmem_limit_bytes=60 * 2**20
        ),
        name=kernel.__name__,
    )(*args)


def target_kernel(teachers, told, out, rows, picks):
    senders, tubes, _ = teachers.shape
    lane = lax.broadcasted_iota(jnp.int32, (1, 128), 1) // 32 * 128
    tube_at = lax.broadcasted_iota(jnp.int32, (tubes, 128), 0)
    cell_at = lax.broadcasted_iota(jnp.int32, (512, 128), 0)

    for half in (0, 1):

        @pl.loop(0, senders)
        def _(s):
            at = pl.ds(pl.multiple_of(s * 128, 128), 128)
            note = told[s]
            tube = note[half : half + 1].astype(jnp.int32)
            cell = note[2 + half : 3 + half].astype(jnp.int32) + lane
            scale = note[4 + half : 5 + half]
            select = jnp.where(tube_at == tube, 1.0, 0.0).astype(jnp.bfloat16)
            rows[at, :] = lax.dot_general(
                select, teachers[s], (((0,), (0,)), ((), ())), preferred_element_type=jnp.float32
            ).astype(jnp.bfloat16)
            picks[:, at] = jnp.where(cell_at == cell, scale, 0.0).astype(jnp.bfloat16)

        out[half * 512 : half * 512 + 512, :] = jnp.dot(
            picks[...], rows[...], preferred_element_type=jnp.float32
        ).astype(jnp.bfloat16)


def tile_kernel(line_s, line_t, column_s, column_t, out, slope):
    count = line_s.shape[0]

    @pl.loop(0, count // 256)
    def _(j):
        at = pl.ds(pl.multiple_of(j * 256, 256), 256)
        gram_s = lax.dot_general(column_s[...], line_s[at, :], NT, preferred_element_type=jnp.float32)
        gram_t = lax.dot_general(column_t[...], line_t[at, :], NT, preferred_element_type=jnp.float32)
        slope[:, at] = jnp.clip((gram_s - gram_t) / huber_delta, -1.0, 1.0).astype(jnp.bfloat16)

    @pl.loop(0, out.shape[0] // 256)
    def _(i):
        at = pl.ds(pl.multiple_of(i * 256, 256), 256)
        out[at, :] = jnp.dot(slope[at, :], line_s[...], preferred_element_type=jnp.float32).astype(
            jnp.bfloat16
        )


def plain(kernel, out, scratch, flops, *args):
    return pl.pallas_call(
        kernel,
        out_shape=jax.ShapeDtypeStruct(out, jnp.bfloat16),
        in_specs=[pl.BlockSpec(memory_space=pltpu.VMEM)] * len(args),
        out_specs=pl.BlockSpec(memory_space=pltpu.VMEM),
        scratch_shapes=[pltpu.VMEM(s, jnp.bfloat16) for s in scratch],
        compiler_params=pltpu.CompilerParams(vmem_limit_bytes=60 * 2**20),
        cost_estimate=pl.CostEstimate(flops=flops, bytes_accessed=2**23, transcendentals=0),
        name=kernel.__name__,
    )(*args)


def notes_of(block_map, block_counts, interp_weights):
    slots, peers = block_map.shape[2], block_counts.shape[1]
    per_peer = slots // peers
    levels = interp_weights.shape[0]
    fields = block_map[0]
    matches = fields[2][:, None] == jnp.arange(levels, dtype=jnp.int32)[None, :]
    weights = jnp.sum(jnp.where(matches, interp_weights[None, :], 0.0), axis=1)
    live = jnp.arange(per_peer, dtype=jnp.int32)[None, :] < block_counts[0][:, None]
    scale = weights * live.reshape(slots).astype(jnp.float32)
    notes = jnp.stack([fields[0].astype(jnp.float32), fields[1].astype(jnp.float32), scale])
    notes = notes.reshape(3, 2, 4, 4, 2, 2, per_peer)
    notes = jnp.stack([notes[:, 0], notes[:, 1, :, :, ::-1]], axis=1)
    notes = notes.transpose(3, 4, 5, 0, 1, 2, 6).reshape(16, 3 * 8 * per_peer // 128, 128)
    return jnp.pad(notes, ((0, 0), (0, 8 - notes.shape[1]), (0, 0)))


def local(student_hidden, projection, teacher, block_map, block_counts, interp_weights):
    tokens, width = student_hidden.shape[0], projection.shape[1]
    tubes = teacher.shape[0]
    bf16, f32 = jnp.bfloat16, jnp.float32
    notes = notes_of(block_map, block_counts, interp_weights)
    proj = jnp.dot(student_hidden, projection, preferred_element_type=f32)
    inverse = lax.rsqrt(jnp.sum(proj * proj, axis=1, keepdims=True) + norm_eps)
    unit = proj * inverse
    student_unit = unit.astype(bf16)

    block = (tokens, width)
    teachers, column_s, told = exchange(
        first_kernel,
        1,
        (((16, tubes, width), bf16), ((8, *block), bf16), ((16, 8, 128), f32)),
        (17, 9, 16),
        teacher,
        student_unit,
        notes,
    )
    parts = plain(
        target_kernel,
        (8 * tokens, width),
        ((2048, width), (512, 2048)),
        5 * 10**9,
        teachers,
        told,
    ).reshape(8, *block)
    line_s, arrived = exchange(
        second_kernel, 2, (((16, *block), bf16), ((8, *block), bf16)), (17, 8), student_unit, parts
    )
    target = jnp.sum(arrived.astype(f32), axis=0)
    teacher_unit = (
        target * lax.rsqrt(jnp.sum(target * target, axis=1, keepdims=True) + norm_eps)
    ).astype(bf16)
    line_t, column_t = exchange(
        third_kernel, 3, (((16, *block), bf16), ((8, *block), bf16)), (17, 9), teacher_unit
    )
    sums = plain(
        tile_kernel,
        (8 * tokens, width),
        ((8 * tokens, 16 * tokens),),
        10**10,
        line_s.reshape(-1, width),
        line_t.reshape(-1, width),
        column_s.reshape(-1, width),
        column_t.reshape(-1, width),
    ).reshape(8, *block)
    (summed,) = exchange(fourth_kernel, 4, (((8, *block), bf16),), (8,), sums)
    grad_unit = 2.0 * jnp.sum(summed.astype(f32), axis=0)
    along = jnp.sum(unit * grad_unit, axis=1, keepdims=True)
    grad_proj = ((grad_unit - unit * along) * inverse).astype(bf16)
    grad_hidden = lax.dot_general(grad_proj, projection, NT, preferred_element_type=f32)
    return grad_hidden.astype(bf16)


def solution(mesh):
    return jax.shard_map(
        local,
        mesh=mesh,
        in_specs=(
            P(BOTH, None),
            P(),
            P(BOTH, None),
            P(BOTH, None, None),
            P(BOTH, None),
            P(),
        ),
        out_specs=P(BOTH, None),
        check_vma=False,
    )
```

```python
import jax
import jax.numpy as jnp
from jax import lax
from jax.experimental import pallas as pl
from jax.experimental.pallas import tpu as pltpu
from jax.sharding import PartitionSpec as P

BOTH = ("row", "col")
MESH = pl.DeviceIdType.MESH
NT = (((1,), (1,)), ((), ()))

huber_delta = 0.05
norm_eps = 1e-06


class Place:
    def __init__(self):
        row, col = lax.axis_index("row"), lax.axis_index("col")
        self.zh, self.y = row // 4, row % 4
        self.x, self.zl, self.core = col // 4, (col // 2) % 2, col % 2

    def row_of(self, d, q):
        return (self.zh + q) % 2 * 4 + (self.y + d) % 4

    def a(self, d, q, k=0):
        col = (self.x + d) % 4 * 4 + (self.zl + q) % 2 * 2 + (self.core + k) % 2
        return (self.zh * 4 + self.y, col)

    def b(self, d, q):
        col = self.x * 4 + (self.zl + q) % 2 * 2 + self.core
        return (self.row_of(d, q), col)


def greet(peers):
    barrier = pltpu.get_barrier_semaphore()
    for peer in peers:
        pl.semaphore_signal(barrier, inc=1, device_id=peer, device_id_type=MESH)
    pl.semaphore_wait(barrier, len(peers))


def remote(src, dst, send, recv, i, device):
    return pltpu.make_async_remote_copy(
        src_ref=src,
        dst_ref=dst,
        send_sem=send.at[i],
        recv_sem=recv.at[i],
        device_id=device,
        device_id_type=MESH,
    )


def rows_of(ref, at, count):
    return ref.at[pl.ds(pl.multiple_of(at, 16), count)]


def gather(own, buf, sems, to, cut, ends, twin=None):
    send, recv = sems
    n = own.shape[0]

    def part(block, start=0, count=n):
        return rows_of(buf, block * n + start, count)

    ahead, behind, across = to(1, 0), to(3, 0), to(0, 1)
    lo, hi = (0, cut), (cut, n - cut)
    plan = [
        (own, part(3), ahead),
        (own, part(1), behind),
        (own, part(4), across),
        (part(3, *lo), part(2, *lo), ahead),
        (part(1, *hi), part(2, *hi), behind),
        (part(4), part(7), ahead),
        (part(4), part(5), behind),
        (part(2, *lo), part(6, *lo), across),
        (part(2, *hi), part(6, *hi), across),
    ]
    copies = [remote(s, d, send, recv, i, dev) for i, (s, d, dev) in enumerate(plan)]
    ends.extend(copies)
    twins = []

    def pass_on(src, block):
        if twin is not None:
            copy = remote(src, part(8 + block), send, recv, 9 + block, twin)
            copy.start()
            twins.append(copy)
            ends.append(copy)

    for i in (0, 1, 2):
        copies[i].start()
    pass_on(own, 0)
    buf[0:n, :] = own[...]
    yield
    after = ((0, (3,), 3), (1, (4,), 1), (2, (5, 6), 4), (3, (7,), None), (4, (8,), 2))
    after += ((5, (), 7), (6, (), 5), (7, (), None), (8, (), 6))
    for i, starts, block in after:
        copies[i].wait_recv()
        for j in starts:
            copies[j].start()
        if block is not None:
            pass_on(part(block), block)
        yield
    for copy in twins:
        copy.wait_recv()


def reduce(blocks, block_of, land, sums, sems, to, ends, total):
    send, recv = sems
    n = total.shape[0]
    half = n // 2
    ahead, behind, across = to(1, 0), to(3, 0), to(0, 1)

    def mine(d, q, start=0, count=n):
        return rows_of(blocks, block_of(d, q) * n + start, count)

    def at(ref, slot, start=0, count=n):
        return rows_of(ref, slot * n + start, count)

    def wide(ref):
        return ref[...].astype(jnp.float32)

    lo, hi = (0, half), (half, half)
    plan = [
        (mine(2, 1), at(land, 0), across),
        (mine(1, 1), at(land, 1), ahead),
        (mine(3, 1), at(land, 2), behind),
        (at(sums, 0, *lo), at(land, 3, *lo), ahead),
        (at(sums, 0, *hi), at(land, 3, *hi), behind),
        (at(sums, 1), at(land, 4), across),
        (mine(1, 0, *hi), at(land, 5, *hi), ahead),
        (at(sums, 2, *lo), at(land, 5, *lo), ahead),
        (mine(3, 0, *lo), at(land, 6, *lo), behind),
        (at(sums, 2, *hi), at(land, 6, *hi), behind),
    ]
    copies = [remote(s, d, send, recv, i, dev) for i, (s, d, dev) in enumerate(plan)]
    ends.extend(copies)

    def store(slot, start, count, *terms):
        value = wide(terms[0])
        for term in terms[1:]:
            value = value + wide(term)
        at(sums, slot, start, count)[...] = value.astype(jnp.bfloat16)

    copies[0].start()
    copies[2].start()
    copies[1].start()
    yield
    copies[6].start()
    copies[8].start()
    yield
    copies[0].wait_recv()
    store(0, 0, n, mine(2, 0), at(land, 0))
    copies[3].start()
    copies[4].start()
    yield
    copies[1].wait_recv()
    copies[2].wait_recv()
    store(1, 0, n, mine(0, 1), at(land, 1), at(land, 2))
    copies[5].start()
    yield
    copies[3].wait_recv()
    store(2, *lo, mine(1, 0, *lo), at(land, 3, *lo))
    copies[7].start()
    copies[4].wait_recv()
    store(2, *hi, mine(3, 0, *hi), at(land, 3, *hi))
    copies[9].start()
    yield
    for i in (6, 8, 5, 7, 9):
        copies[i].wait_recv()
    total[...] = wide(mine(0, 0)) + wide(at(land, 4)) + wide(at(land, 5)) + wide(at(land, 6))


def step(*plans):
    for plan in plans:
        next(plan, None)


def finish(*plans):
    plans = list(plans)
    while plans:
        for plan in list(plans):
            try:
                next(plan)
            except StopIteration:
                plans.remove(plan)


def whole_kernel(
    teacher, own_s, notes, total,
    teachers, told, rows, picks, parts, line_s, column_s, line_t, column_t, own_t, gram, slope,
    land_0, sums_0, land_1, sums_1, *sems,
):
    f32, bf16 = jnp.float32, jnp.bfloat16
    pairs = [sems[i : i + 2] for i in range(0, len(sems), 2)]
    me = Place()
    twin = me.a(0, 0, 1)
    tubes, tokens = teacher.shape[0], own_s.shape[0]
    others = [(d, q, k) for k in (0, 1) for q in (0, 1) for d in range(4) if d or q or k]
    greet([me.a(*o) for o in others] + [me.b(1, 0), me.b(3, 0), me.b(0, 1)])
    ends = []

    teach = gather(teacher, teachers, pairs[0], me.a, 48, ends, twin)
    step(teach)
    told_by = []
    for d, q, k in others:
        twist = (me.zh + me.zl + q) % 2
        note = (me.x + d) % 4 * 4 + twist * 2 + (me.core + k) % 2
        slot = k * 8 + q * 4 + (4 - d) % 4
        copy = remote(notes.at[note], told.at[slot], *pairs[1], slot, me.a(d, q, k))
        copy.start()
        told_by.append(copy)
        ends.append(copy)
    told[0] = notes[me.x * 4 + (me.zh + me.zl) % 2 * 2 + me.core]
    spread = gather(own_s, column_s, pairs[2], me.b, 64, ends)
    step(spread)
    for _ in range(5):
        step(teach, spread)
    align = gather(own_s, line_s, pairs[3], me.a, 64, ends, twin)
    step(align)
    for copy in told_by:
        copy.wait_recv()
    finish(teach, spread)

    lane = lax.broadcasted_iota(jnp.int32, (1, 128), 1) // 32 * 128
    tube_at = lax.broadcasted_iota(jnp.int32, (tubes, 128), 0)
    cell_at = lax.broadcasted_iota(jnp.int32, (4 * tokens, 128), 0)

    def weigh(first, last):
        @pl.loop(first, last)
        def _(s):
            at = pl.ds(pl.multiple_of(s * 128, 128), 128)
            note = told[s]
            features = teachers[pl.ds(pl.multiple_of(s * tubes, 16), tubes), :]
            for half in (0, 1):
                tube = note[half : half + 1].astype(jnp.int32)
                cell = note[2 + half : 3 + half].astype(jnp.int32) + lane
                scale = note[4 + half : 5 + half]
                select = jnp.where(tube_at == tube, 1.0, 0.0).astype(bf16)
                rows[half, at, :] = lax.dot_general(
                    select, features, (((0,), (0,)), ((), ())), preferred_element_type=f32
                ).astype(bf16)
                picks[half, :, at] = jnp.where(cell_at == cell, scale, 0.0).astype(bf16)

    def add_up(half):
        at = pl.ds(pl.multiple_of(half * 4 * tokens, 128), 4 * tokens)
        parts[at, :] = jnp.dot(picks[half], rows[half], preferred_element_type=f32).astype(bf16)

    weigh(0, 8)
    step(align)
    weigh(8, 16)
    step(align)
    merge = reduce(parts, me.row_of, land_0, sums_0, pairs[4], me.b, ends, total)
    add_up((me.zh + 1) % 2)
    step(merge, align)
    add_up(me.zh)
    finish(merge, align)
    target = total[...]
    own_t[...] = (
        target * lax.rsqrt(jnp.sum(target * target, axis=1, keepdims=True) + norm_eps)
    ).astype(bf16)

    line = gather(own_t, line_t, pairs[5], me.a, 64, ends, twin)
    column = gather(own_t, column_t, pairs[6], me.b, 64, ends)
    step(line, column)
    wide = 256

    def student(first, last):
        @pl.loop(first, last)
        def _(j):
            at = pl.ds(pl.multiple_of(j * wide, wide), wide)
            gram[:, at] = lax.dot_general(
                column_s[...], line_s[at, :], NT, preferred_element_type=f32
            )

    student(0, 4)
    for j in range(4, 8):
        step(line, column)
        student(j, j + 1)
    finish(line, column)

    @pl.loop(0, 16 * tokens // wide)
    def _(j):
        at = pl.ds(pl.multiple_of(j * wide, wide), wide)
        gram_t = lax.dot_general(column_t[...], line_t[at, :], NT, preferred_element_type=f32)
        slope[:, at] = jnp.clip((gram[:, at] - gram_t) * (1.0 / huber_delta), -1.0, 1.0).astype(bf16)

    def pull(first, last):
        @pl.loop(first, last)
        def _(i):
            at = pl.ds(pl.multiple_of(i * wide, wide), wide)
            parts[at, :] = jnp.dot(slope[at, :], line_s[...], preferred_element_type=f32).astype(bf16)

    for copy in ends:
        copy.wait_send()
    ends.clear()
    merge = reduce(
        parts, lambda d, q: q * 4 + d, land_1, sums_1, pairs[7], me.b, ends, total
    )
    pull(2, 4)
    step(merge)
    pull(0, 2)
    finish(merge)
    for copy in ends:
        copy.wait_send()


def whole(teacher, own, notes):
    tubes, (tokens, width) = teacher.shape[0], own.shape
    f32, bf16 = jnp.float32, jnp.bfloat16
    buffers = (
        ((16 * tubes, width), bf16),
        ((16, 8, 128), f32),
        ((2, 2048, width), bf16),
        ((2, 4 * tokens, 2048), bf16),
        ((8 * tokens, width), bf16),
        ((16 * tokens, width), bf16),
        ((8 * tokens, width), bf16),
        ((16 * tokens, width), bf16),
        ((8 * tokens, width), bf16),
        ((tokens, width), bf16),
        ((8 * tokens, 16 * tokens), f32),
        ((8 * tokens, 16 * tokens), bf16),
        ((7 * tokens, width), bf16),
        ((3 * tokens, width), bf16),
        ((7 * tokens, width), bf16),
        ((3 * tokens, width), bf16),
    )
    sems = (17, 16, 9, 17, 10, 17, 9, 10)
    return pl.pallas_call(
        whole_kernel,
        out_shape=jax.ShapeDtypeStruct((tokens, width), f32),
        in_specs=[pl.BlockSpec(memory_space=pltpu.VMEM)] * 3,
        out_specs=pl.BlockSpec(memory_space=pltpu.VMEM),
        scratch_shapes=[pltpu.VMEM(*b) for b in buffers]
        + [pltpu.SemaphoreType.DMA((n,)) for n in sems for _ in (0, 1)],
        compiler_params=pltpu.CompilerParams(
            collective_id=1, has_side_effects=True, vmem_limit_bytes=60 * 2**20
        ),
        name="whole_kernel",
    )(teacher, own, notes)


def notes_of(block_map, block_counts, interp_weights):
    slots, peers = block_map.shape[2], block_counts.shape[1]
    per_peer = slots // peers
    levels = interp_weights.shape[0]
    fields = block_map[0]
    matches = fields[2][:, None] == jnp.arange(levels, dtype=jnp.int32)[None, :]
    weights = jnp.sum(jnp.where(matches, interp_weights[None, :], 0.0), axis=1)
    live = jnp.arange(per_peer, dtype=jnp.int32)[None, :] < block_counts[0][:, None]
    scale = weights * live.reshape(slots).astype(jnp.float32)
    notes = jnp.stack([fields[0].astype(jnp.float32), fields[1].astype(jnp.float32), scale])
    notes = notes.reshape(3, 2, 4, 4, 2, 2, per_peer)
    notes = jnp.stack([notes[:, 0], notes[:, 1, :, :, ::-1]], axis=1)
    notes = notes.transpose(3, 4, 5, 0, 1, 2, 6).reshape(16, 3 * 8 * per_peer // 128, 128)
    return jnp.pad(notes, ((0, 0), (0, 8 - notes.shape[1]), (0, 0)))


def local(student_hidden, projection, teacher, block_map, block_counts, interp_weights):
    bf16, f32 = jnp.bfloat16, jnp.float32
    notes = notes_of(block_map, block_counts, interp_weights)
    proj = jnp.dot(student_hidden, projection, preferred_element_type=f32)
    inverse = lax.rsqrt(jnp.sum(proj * proj, axis=1, keepdims=True) + norm_eps)
    unit = proj * inverse
    student_unit = unit.astype(bf16)

    grad_unit = 2.0 * whole(teacher, student_unit, notes)
    along = jnp.sum(unit * grad_unit, axis=1, keepdims=True)
    grad_proj = ((grad_unit - unit * along) * inverse).astype(bf16)
    grad_hidden = lax.dot_general(grad_proj, projection, NT, preferred_element_type=f32)
    return grad_hidden.astype(bf16)


def solution(mesh):
    return jax.shard_map(
        local,
        mesh=mesh,
        in_specs=(
            P(BOTH, None),
            P(),
            P(BOTH, None),
            P(BOTH, None, None),
            P(BOTH, None),
            P(),
        ),
        out_specs=P(BOTH, None),
        check_vma=False,
    )
```

```python
import jax
import jax.numpy as jnp
from jax import lax
from jax.experimental import pallas as pl
from jax.experimental.pallas import tpu as pltpu
from jax.sharding import PartitionSpec as P

BOTH = ("row", "col")
MESH = pl.DeviceIdType.MESH
NT = (((1,), (1,)), ((), ()))

huber_delta = 0.05
norm_eps = 1e-06


class Place:
    def __init__(self):
        row, col = lax.axis_index("row"), lax.axis_index("col")
        self.zh, self.y = row // 4, row % 4
        self.x, self.zl, self.core = col // 4, (col // 2) % 2, col % 2

    def row_of(self, d, q):
        return (self.zh + q) % 2 * 4 + (self.y + d) % 4

    def a(self, d, q, k=0):
        col = (self.x + d) % 4 * 4 + (self.zl + q) % 2 * 2 + (self.core + k) % 2
        return (self.zh * 4 + self.y, col)

    def b(self, d, q):
        col = self.x * 4 + (self.zl + q) % 2 * 2 + self.core
        return (self.row_of(d, q), col)


def greet(peers):
    barrier = pltpu.get_barrier_semaphore()
    for peer in peers:
        pl.semaphore_signal(barrier, inc=1, device_id=peer, device_id_type=MESH)
    pl.semaphore_wait(barrier, len(peers))


def remote(src, dst, send, recv, i, device):
    return pltpu.make_async_remote_copy(
        src_ref=src,
        dst_ref=dst,
        send_sem=send.at[i],
        recv_sem=recv.at[i],
        device_id=device,
        device_id_type=MESH,
    )


def rows_of(ref, at, count):
    return ref.at[pl.ds(pl.multiple_of(at, 16), count)]


def gather(own, buf, sems, to, cut, ends, twin=None, off=0, n=None):
    send, recv = sems
    size = own.shape[0]
    n = n or size
    own = rows_of(own, off, n)

    def part(block, start=0, count=n):
        return rows_of(buf, block * size + off + start, count)

    ahead, behind, across = to(1, 0), to(3, 0), to(0, 1)
    lo, hi = (0, cut), (cut, n - cut)
    plan = [
        (own, part(3), ahead),
        (own, part(1), behind),
        (own, part(4), across),
        (part(3, *lo), part(2, *lo), ahead),
        (part(1, *hi), part(2, *hi), behind),
        (part(4), part(7), ahead),
        (part(4), part(5), behind),
        (part(2, *lo), part(6, *lo), across),
        (part(2, *hi), part(6, *hi), across),
    ]
    copies = [remote(s, d, send, recv, i, dev) for i, (s, d, dev) in enumerate(plan)]
    ends.extend(copies)
    twins = []

    def pass_on(src, block):
        if twin is not None:
            copy = remote(src, part(8 + block), send, recv, 9 + block, twin)
            copy.start()
            twins.append(copy)
            ends.append(copy)

    for i in (0, 1, 2):
        copies[i].start()
    pass_on(own, 0)
    buf[off : off + n, :] = own[...]
    yield
    after = ((0, (3,), 3), (1, (4,), 1), (2, (5, 6), 4), (3, (7,), None), (4, (8,), 2))
    after += ((5, (), 7), (6, (), 5), (7, (), None), (8, (), 6))
    for i, starts, block in after:
        copies[i].wait_recv()
        for j in starts:
            copies[j].start()
        if block is not None:
            pass_on(part(block), block)
        yield
    for copy in twins:
        copy.wait_recv()


def reduce(blocks, block_of, land, sums, sems, to, ends, total, off=0, n=None):
    send, recv = sems
    size = total.shape[0]
    n = n or size
    half = n // 2
    ahead, behind, across = to(1, 0), to(3, 0), to(0, 1)

    def mine(d, q, start=0, count=n):
        return rows_of(blocks, block_of(d, q) * size + off + start, count)

    def at(ref, slot, start=0, count=n):
        return rows_of(ref, slot * size + off + start, count)

    def wide(ref):
        return ref[...].astype(jnp.float32)

    lo, hi = (0, half), (half, half)
    plan = [
        (mine(2, 1), at(land, 0), across),
        (mine(1, 1), at(land, 1), ahead),
        (mine(3, 1), at(land, 2), behind),
        (at(sums, 0, *lo), at(land, 3, *lo), ahead),
        (at(sums, 0, *hi), at(land, 3, *hi), behind),
        (at(sums, 1), at(land, 4), across),
        (mine(1, 0, *hi), at(land, 5, *hi), ahead),
        (at(sums, 2, *lo), at(land, 5, *lo), ahead),
        (mine(3, 0, *lo), at(land, 6, *lo), behind),
        (at(sums, 2, *hi), at(land, 6, *hi), behind),
    ]
    copies = [remote(s, d, send, recv, i, dev) for i, (s, d, dev) in enumerate(plan)]
    ends.extend(copies)

    def store(slot, start, count, *terms):
        value = wide(terms[0])
        for term in terms[1:]:
            value = value + wide(term)
        at(sums, slot, start, count)[...] = value.astype(jnp.bfloat16)

    copies[0].start()
    copies[2].start()
    yield
    copies[1].start()
    yield
    copies[6].start()
    copies[8].start()
    yield
    copies[0].wait_recv()
    store(0, 0, n, mine(2, 0), at(land, 0))
    copies[3].start()
    copies[4].start()
    yield
    copies[1].wait_recv()
    copies[2].wait_recv()
    store(1, 0, n, mine(0, 1), at(land, 1), at(land, 2))
    copies[5].start()
    yield
    copies[3].wait_recv()
    store(2, *lo, mine(1, 0, *lo), at(land, 3, *lo))
    copies[7].start()
    copies[4].wait_recv()
    store(2, *hi, mine(3, 0, *hi), at(land, 3, *hi))
    copies[9].start()
    yield
    for i in (6, 8, 5, 7, 9):
        copies[i].wait_recv()
    landed = wide(at(land, 4)) + wide(at(land, 5)) + wide(at(land, 6))
    total[off : off + n, :] = wide(mine(0, 0)) + landed


def step(*plans):
    for plan in plans:
        next(plan, None)


def steps(count, *plans):
    for _ in range(count):
        step(*plans)


def finish(*plans):
    plans = list(plans)
    while plans:
        for plan in list(plans):
            try:
                next(plan)
            except StopIteration:
                plans.remove(plan)


def write_notes(block_map, block_counts, interp_weights, before, notes):
    f32, i32 = jnp.float32, jnp.int32
    for y in range(4):
        for x in range(4):
            for zh in (0, 1):
                chunk = (zh * 4 + y) * 4 + x
                row = y * 8 + x * 2 + zh
                for field in range(3):
                    before[field, row : row + 1, :] = block_map[field, chunk : chunk + 1, :]
    row = lax.broadcasted_iota(i32, (32, 128), 0)
    column = lax.broadcasted_iota(i32, (32, 128), 1)
    chunk = (row % 2 * 4 + row // 8) * 4 + row % 8 // 2
    counts = jnp.where(column // 4 == chunk, block_counts[...], 0).astype(f32).astype(jnp.bfloat16)
    source = lax.broadcasted_iota(i32, (128, 128), 0)
    lane = lax.broadcasted_iota(i32, (128, 128), 1)
    spread = jnp.where(source % 4 == lane // 32, 1.0, 0.0).astype(jnp.bfloat16)
    counts = jnp.dot(counts, spread, preferred_element_type=f32).astype(i32)
    level = before[2]
    scale = jnp.zeros((32, 128), f32)
    for l in range(interp_weights.shape[0]):
        scale = jnp.where(level == l, interp_weights[l], scale)
    scale = jnp.where(column % 32 < counts, scale, 0.0)
    notes[...] = jnp.zeros_like(notes)
    for field, value in enumerate((before[0].astype(f32), before[1].astype(f32), scale)):
        for g in range(4):
            pieces = [value[y * 8 : y * 8 + 8, g * 32 : g * 32 + 32] for y in range(4)]
            turned = jnp.concatenate(pieces, axis=1)
            for x in range(4):
                for zh in (0, 1):
                    note = x * 4 + (g // 2 + zh) % 2 * 2 + g % 2
                    at = field * 2 + zh
                    notes[note, at : at + 1, :] = turned[x * 2 + zh : x * 2 + zh + 1]


def whole_kernel(
    hidden_in, projection_in, teacher, block_map, block_counts, interp_weights, out,
    hidden, projection, before, notes, unit, total, own_s,
    teachers, told, rows, picks, parts, line_s, column_s, line_t, column_t, own_t, gram, slope,
    land_0, sums_0, land_1, sums_1, loads, *sems,
):
    f32, bf16 = jnp.float32, jnp.bfloat16
    pairs = [sems[i : i + 2] for i in range(0, len(sems), 2)]
    me = Place()
    twin = me.a(0, 0, 1)
    tubes, tokens = teacher.shape[0], own_s.shape[0]
    load_hidden = pltpu.make_async_copy(hidden_in, hidden, loads.at[0])
    load_projection = pltpu.make_async_copy(projection_in, projection, loads.at[1])
    load_hidden.start()
    load_projection.start()
    others = [(d, q, k) for k in (0, 1) for q in (0, 1) for d in range(4) if d or q or k]
    greet([me.a(*o) for o in others] + [me.b(1, 0), me.b(3, 0), me.b(0, 1)])
    ends = []

    teach = gather(teacher, teachers, pairs[0], me.a, 48, ends, twin)
    step(teach)
    write_notes(block_map, block_counts, interp_weights, before, notes)
    told_by = []
    for d, q, k in others:
        twist = (me.zh + me.zl + q) % 2
        note = (me.x + d) % 4 * 4 + twist * 2 + (me.core + k) % 2
        slot = k * 8 + q * 4 + (4 - d) % 4
        copy = remote(notes.at[note], told.at[slot], *pairs[1], slot, me.a(d, q, k))
        copy.start()
        told_by.append(copy)
        ends.append(copy)
    told[0] = notes[me.x * 4 + (me.zh + me.zl) % 2 * 2 + me.core]
    load_hidden.wait()
    load_projection.wait()
    proj = jnp.dot(hidden[...], projection[...], preferred_element_type=f32)
    inverse = lax.rsqrt(jnp.sum(proj * proj, axis=1, keepdims=True) + norm_eps)
    unit[...] = proj * inverse
    own_s[...] = (proj * inverse).astype(bf16)
    spread = gather(own_s, column_s, pairs[2], me.b, 64, ends)
    step(spread)
    steps(5, teach)
    align = gather(own_s, line_s, pairs[3], me.a, 64, ends, twin)
    step(align)
    for copy in told_by:
        copy.wait_recv()

    lane = lax.broadcasted_iota(jnp.int32, (1, 128), 1) // 32 * 128
    tube_at = lax.broadcasted_iota(jnp.int32, (tubes, 128), 0)
    cell_at = lax.broadcasted_iota(jnp.int32, (4 * tokens, 128), 0)

    def weigh(first, last):
        @pl.loop(first, last)
        def _(s):
            at = pl.ds(pl.multiple_of(s * 128, 128), 128)
            note = told[s]
            features = teachers[pl.ds(pl.multiple_of(s * tubes, 16), tubes), :]
            for half in (0, 1):
                tube = note[half : half + 1].astype(jnp.int32)
                cell = note[2 + half : 3 + half].astype(jnp.int32) + lane
                scale = note[4 + half : 5 + half]
                select = jnp.where(tube_at == tube, 1.0, 0.0).astype(bf16)
                rows[half, at, :] = lax.dot_general(
                    select, features, (((0,), (0,)), ((), ())), preferred_element_type=f32
                ).astype(bf16)
                picks[half, :, at] = jnp.where(cell_at == cell, scale, 0.0).astype(bf16)

    def add_up(half):
        at = pl.ds(pl.multiple_of(half * 4 * tokens, 128), 4 * tokens)
        parts[at, :] = jnp.dot(picks[half], rows[half], preferred_element_type=f32).astype(bf16)

    half = tokens // 2
    halves = [dict(off=i * half, n=half) for i in (0, 1)]
    weigh(0, 5)
    steps(3, spread)
    finish(teach)
    weigh(5, 16)
    steps(2, spread)
    steps(3, align)
    merges = [
        reduce(parts, me.row_of, land_0, sums_0, pair, me.b, ends, total, **where)
        for pair, where in zip(pairs[8:10], halves)
    ]
    add_up((me.zh + 1) % 2)
    steps(2, *merges)
    add_up(me.zh)
    step(*merges)
    steps(2, align)
    finish(spread)
    for merge in merges:
        steps(2, merge)
    finish(*merges)
    target = total[...]
    own_t[...] = (
        target * lax.rsqrt(jnp.sum(target * target, axis=1, keepdims=True) + norm_eps)
    ).astype(bf16)

    moves = [
        (
            gather(own_t, line_t, pairs[4 + 2 * i], me.a, half // 2, ends, twin, **where),
            gather(own_t, column_t, pairs[5 + 2 * i], me.b, half // 2, ends, **where),
        )
        for i, where in enumerate(halves)
    ]
    for move in moves:
        step(*move)
    finish(align)
    wide = 256

    def student(first, last):
        @pl.loop(first, last)
        def _(j):
            at = pl.ds(pl.multiple_of(j * wide, wide), wide)
            gram[:, at] = lax.dot_general(
                column_s[...], line_s[at, :], NT, preferred_element_type=f32
            )

    student(0, 4)
    steps(3, *moves[0])
    student(4, 6)
    steps(3, *moves[1])
    steps(2, *moves[0])
    student(6, 8)
    steps(2, *moves[1])
    finish(*moves[0])
    finish(*moves[1])

    @pl.loop(0, 16 * tokens // wide)
    def _(j):
        at = pl.ds(pl.multiple_of(j * wide, wide), wide)
        gram_t = lax.dot_general(column_t[...], line_t[at, :], NT, preferred_element_type=f32)
        slope[:, at] = jnp.clip((gram[:, at] - gram_t) * (1.0 / huber_delta), -1.0, 1.0).astype(bf16)

    def pull(first, last):
        @pl.loop(first, last)
        def _(i):
            at = pl.ds(pl.multiple_of(i * wide, wide), wide)
            parts[at, :] = jnp.dot(slope[at, :], line_s[...], preferred_element_type=f32).astype(bf16)

    for copy in ends:
        copy.wait_send()
    ends.clear()
    merges = [
        reduce(parts, lambda d, q: q * 4 + d, land_1, sums_1, pair, me.b, ends, total, **where)
        for pair, where in zip(pairs[10:12], halves)
    ]
    pull(3, 4)
    step(*merges)
    pull(2, 3)
    step(*merges)
    pull(0, 2)
    step(*merges)
    for merge in merges:
        steps(2, merge)
    finish(*merges)
    grad_unit = 2.0 * total[...]
    along = jnp.sum(unit[...] * grad_unit, axis=1, keepdims=True)
    out[...] = ((grad_unit - unit[...] * along) * inverse).astype(bf16)
    for copy in ends:
        copy.wait_send()


def local(student_hidden, projection, teacher, block_map, block_counts, interp_weights):
    (tokens, depth), width = student_hidden.shape, projection.shape[1]
    tubes = teacher.shape[0]
    f32, bf16, i32 = jnp.float32, jnp.bfloat16, jnp.int32
    buffers = (
        ((tokens, depth), bf16),
        ((depth, width), bf16),
        ((3, 32, 128), i32),
        ((16, 8, 128), f32),
        ((tokens, width), f32),
        ((tokens, width), f32),
        ((tokens, width), bf16),
        ((16 * tubes, width), bf16),
        ((16, 8, 128), f32),
        ((2, 2048, width), bf16),
        ((2, 4 * tokens, 2048), bf16),
        ((8 * tokens, width), bf16),
        ((16 * tokens, width), bf16),
        ((8 * tokens, width), bf16),
        ((16 * tokens, width), bf16),
        ((8 * tokens, width), bf16),
        ((tokens, width), bf16),
        ((8 * tokens, 16 * tokens), f32),
        ((8 * tokens, 16 * tokens), bf16),
        ((7 * tokens, width), bf16),
        ((3 * tokens, width), bf16),
        ((7 * tokens, width), bf16),
        ((3 * tokens, width), bf16),
    )
    sems = (17, 16, 9, 17, 17, 9, 17, 9, 10, 10, 10, 10)
    fields = block_map.reshape(3, -1, 128)
    kept = pl.BlockSpec(memory_space=pltpu.VMEM)
    left = pl.BlockSpec(memory_space=pl.ANY)
    grad_proj = pl.pallas_call(
        whole_kernel,
        out_shape=jax.ShapeDtypeStruct((tokens, width), bf16),
        in_specs=[left, left, kept, kept, kept, pl.BlockSpec(memory_space=pltpu.SMEM)],
        out_specs=kept,
        scratch_shapes=[pltpu.VMEM(*b) for b in buffers]
        + [pltpu.SemaphoreType.DMA((2,))]
        + [pltpu.SemaphoreType.DMA((n,)) for n in sems for _ in (0, 1)],
        compiler_params=pltpu.CompilerParams(
            collective_id=1, has_side_effects=True, vmem_limit_bytes=60 * 2**20
        ),
        name="whole_kernel",
    )(student_hidden, projection, teacher, fields, block_counts, interp_weights)
    grad_hidden = lax.dot_general(grad_proj, projection, NT, preferred_element_type=f32)
    return grad_hidden.astype(bf16)


def solution(mesh):
    return jax.shard_map(
        local,
        mesh=mesh,
        in_specs=(
            P(BOTH, None),
            P(),
            P(BOTH, None),
            P(BOTH, None, None),
            P(BOTH, None),
            P(),
        ),
        out_specs=P(BOTH, None),
        check_vma=False,
    )
```

```python
import jax
import jax.numpy as jnp
from jax import lax
from jax.experimental import pallas as pl
from jax.experimental.pallas import tpu as pltpu
from jax.sharding import PartitionSpec as P

BOTH = ("row", "col")
MESH = pl.DeviceIdType.MESH
NT = (((1,), (1,)), ((), ()))

huber_delta = 0.05
norm_eps = 1e-06


class Place:
    def __init__(self):
        row, col = lax.axis_index("row"), lax.axis_index("col")
        self.zh, self.y = row // 4, row % 4
        self.x, self.zl, self.core = col // 4, (col // 2) % 2, col % 2

    def row_of(self, d, q):
        return (self.zh + q) % 2 * 4 + (self.y + d) % 4

    def a(self, d, q, k=0):
        col = (self.x + d) % 4 * 4 + (self.zl + q) % 2 * 2 + (self.core + k) % 2
        return (self.zh * 4 + self.y, col)

    def b(self, d, q):
        col = self.x * 4 + (self.zl + q) % 2 * 2 + self.core
        return (self.row_of(d, q), col)


def greet(peers):
    barrier = pltpu.get_barrier_semaphore()
    for peer in peers:
        pl.semaphore_signal(barrier, inc=1, device_id=peer, device_id_type=MESH)
    pl.semaphore_wait(barrier, len(peers))


def remote(src, dst, send, recv, i, device):
    return pltpu.make_async_remote_copy(
        src_ref=src,
        dst_ref=dst,
        send_sem=send.at[i],
        recv_sem=recv.at[i],
        device_id=device,
        device_id_type=MESH,
    )


def rows_of(ref, at, count):
    return ref.at[pl.ds(pl.multiple_of(at, 16), count)]


def gather(own, buf, sems, to, cut, ends, twin=None, off=0, n=None):
    send, recv = sems
    size = own.shape[0]
    n = n or size
    own = rows_of(own, off, n)

    def part(block, start=0, count=n):
        return rows_of(buf, block * size + off + start, count)

    ahead, behind, across = to(1, 0), to(3, 0), to(0, 1)
    lo, hi = (0, cut), (cut, n - cut)
    plan = [
        (own, part(3), ahead),
        (own, part(1), behind),
        (own, part(4), across),
        (part(3, *lo), part(2, *lo), ahead),
        (part(1, *hi), part(2, *hi), behind),
        (part(4), part(7), ahead),
        (part(4), part(5), behind),
        (part(2, *lo), part(6, *lo), across),
        (part(2, *hi), part(6, *hi), across),
    ]
    copies = [remote(s, d, send, recv, i, dev) for i, (s, d, dev) in enumerate(plan)]
    ends.extend(copies)
    twins = []

    def pass_on(src, block):
        if twin is not None:
            copy = remote(src, part(8 + block), send, recv, 9 + block, twin)
            copy.start()
            twins.append(copy)
            ends.append(copy)

    for i in (0, 1, 2):
        copies[i].start()
    pass_on(own, 0)
    buf[off : off + n, :] = own[...]
    yield
    after = ((0, (3,), 3), (1, (4,), 1), (2, (5, 6), 4), (3, (7,), None), (4, (8,), 2))
    after += ((5, (), 7), (6, (), 5), (7, (), None), (8, (), 6))
    for i, starts, block in after:
        copies[i].wait_recv()
        for j in starts:
            copies[j].start()
        if block is not None:
            pass_on(part(block), block)
        yield
    for copy in twins:
        copy.wait_recv()


def reduce(blocks, block_of, land, sums, sems, to, ends, total, off=0, n=None):
    send, recv = sems
    size = total.shape[0]
    n = n or size
    half = n // 2
    ahead, behind, across = to(1, 0), to(3, 0), to(0, 1)

    def mine(d, q, start=0, count=n):
        return rows_of(blocks, block_of(d, q) * size + off + start, count)

    def at(ref, slot, start=0, count=n):
        return rows_of(ref, slot * size + off + start, count)

    def wide(ref):
        return ref[...].astype(jnp.float32)

    lo, hi = (0, half), (half, half)
    plan = [
        (mine(2, 1), at(land, 0), across),
        (mine(1, 1), at(land, 1), ahead),
        (mine(3, 1), at(land, 2), behind),
        (at(sums, 0, *lo), at(land, 3, *lo), ahead),
        (at(sums, 0, *hi), at(land, 3, *hi), behind),
        (at(sums, 1), at(land, 4), across),
        (mine(1, 0, *hi), at(land, 5, *hi), ahead),
        (at(sums, 2, *lo), at(land, 5, *lo), ahead),
        (mine(3, 0, *lo), at(land, 6, *lo), behind),
        (at(sums, 2, *hi), at(land, 6, *hi), behind),
    ]
    copies = [remote(s, d, send, recv, i, dev) for i, (s, d, dev) in enumerate(plan)]
    ends.extend(copies)

    def store(slot, start, count, *terms):
        value = wide(terms[0])
        for term in terms[1:]:
            value = value + wide(term)
        at(sums, slot, start, count)[...] = value.astype(jnp.bfloat16)

    copies[0].start()
    copies[2].start()
    yield
    copies[1].start()
    yield
    copies[0].wait_recv()
    store(0, 0, n, mine(2, 0), at(land, 0))
    copies[3].start()
    copies[4].start()
    copies[6].start()
    copies[8].start()
    yield
    copies[1].wait_recv()
    copies[2].wait_recv()
    store(1, 0, n, mine(0, 1), at(land, 1), at(land, 2))
    copies[5].start()
    yield
    copies[3].wait_recv()
    store(2, *lo, mine(1, 0, *lo), at(land, 3, *lo))
    copies[7].start()
    copies[4].wait_recv()
    store(2, *hi, mine(3, 0, *hi), at(land, 3, *hi))
    copies[9].start()
    yield
    for i in (6, 8, 5, 7, 9):
        copies[i].wait_recv()
    landed = wide(at(land, 4)) + wide(at(land, 5)) + wide(at(land, 6))
    total[off : off + n, :] = wide(mine(0, 0)) + landed


def step(*plans):
    for plan in plans:
        next(plan, None)


def steps(count, *plans):
    for _ in range(count):
        step(*plans)


def finish(*plans):
    plans = list(plans)
    while plans:
        for plan in list(plans):
            try:
                next(plan)
            except StopIteration:
                plans.remove(plan)


def write_notes(block_map, block_counts, interp_weights, before, notes):
    f32, i32 = jnp.float32, jnp.int32
    for y in range(4):
        for x in range(4):
            for zh in (0, 1):
                chunk = (zh * 4 + y) * 4 + x
                row = y * 8 + x * 2 + zh
                for field in range(3):
                    before[field, row : row + 1, :] = block_map[field, chunk : chunk + 1, :]
    row = lax.broadcasted_iota(i32, (32, 128), 0)
    column = lax.broadcasted_iota(i32, (32, 128), 1)
    chunk = (row % 2 * 4 + row // 8) * 4 + row % 8 // 2
    counts = jnp.where(column // 4 == chunk, block_counts[...], 0).astype(f32).astype(jnp.bfloat16)
    source = lax.broadcasted_iota(i32, (128, 128), 0)
    lane = lax.broadcasted_iota(i32, (128, 128), 1)
    spread = jnp.where(source % 4 == lane // 32, 1.0, 0.0).astype(jnp.bfloat16)
    counts = jnp.dot(counts, spread, preferred_element_type=f32).astype(i32)
    level = before[2]
    scale = jnp.zeros((32, 128), f32)
    for l in range(interp_weights.shape[0]):
        scale = jnp.where(level == l, interp_weights[l], scale)
    scale = jnp.where(column % 32 < counts, scale, 0.0)
    notes[...] = jnp.zeros_like(notes)
    for field, value in enumerate((before[0].astype(f32), before[1].astype(f32), scale)):
        for g in range(4):
            pieces = [value[y * 8 : y * 8 + 8, g * 32 : g * 32 + 32] for y in range(4)]
            turned = jnp.concatenate(pieces, axis=1)
            for x in range(4):
                for zh in (0, 1):
                    note = x * 4 + (g // 2 + zh) % 2 * 2 + g % 2
                    at = field * 2 + zh
                    notes[note, at : at + 1, :] = turned[x * 2 + zh : x * 2 + zh + 1]


def whole_kernel(
    hidden_in, projection_in, teacher, block_map, block_counts, interp_weights, out,
    hidden, projection, before, notes, unit, total, own_s,
    teachers, told, rows, picks, parts, line_s, column_s, line_t, column_t, own_t, gram, slope,
    land_0, sums_0, land_1, sums_1, loads, *sems,
):
    f32, bf16 = jnp.float32, jnp.bfloat16
    pairs = [sems[i : i + 2] for i in range(0, len(sems), 2)]
    me = Place()
    twin = me.a(0, 0, 1)
    tubes, tokens = teacher.shape[0], own_s.shape[0]
    load_hidden = pltpu.make_async_copy(hidden_in, hidden, loads.at[0])
    load_projection = pltpu.make_async_copy(projection_in, projection, loads.at[1])
    load_hidden.start()
    load_projection.start()
    others = [(d, q, k) for k in (0, 1) for q in (0, 1) for d in range(4) if d or q or k]
    greet([me.a(*o) for o in others] + [me.b(1, 0), me.b(3, 0), me.b(0, 1)])
    ends = []

    teach = gather(teacher, teachers, pairs[0], me.a, 48, ends, twin)
    step(teach)
    write_notes(block_map, block_counts, interp_weights, before, notes)
    told_by = []
    for d, q, k in others:
        twist = (me.zh + me.zl + q) % 2
        note = (me.x + d) % 4 * 4 + twist * 2 + (me.core + k) % 2
        slot = k * 8 + q * 4 + (4 - d) % 4
        copy = remote(notes.at[note], told.at[slot], *pairs[1], slot, me.a(d, q, k))
        copy.start()
        told_by.append(copy)
        ends.append(copy)
    told[0] = notes[me.x * 4 + (me.zh + me.zl) % 2 * 2 + me.core]
    load_hidden.wait()
    load_projection.wait()
    proj = jnp.dot(hidden[...], projection[...], preferred_element_type=f32)
    inverse = lax.rsqrt(jnp.sum(proj * proj, axis=1, keepdims=True) + norm_eps)
    unit[...] = proj * inverse
    own_s[...] = (proj * inverse).astype(bf16)
    spread = gather(own_s, column_s, pairs[2], me.b, 64, ends)
    step(spread)
    steps(3, teach)
    for copy in told_by:
        copy.wait_recv()

    lane = lax.broadcasted_iota(jnp.int32, (1, 128), 1) // 32 * 128
    tube_at = lax.broadcasted_iota(jnp.int32, (tubes, 256), 0)
    cell_at = lax.broadcasted_iota(jnp.int32, (4 * tokens, 128), 0)

    @pl.loop(0, 16)
    def _(s):
        at = pl.ds(pl.multiple_of(s * 128, 128), 128)
        note = told[s]
        for half in (0, 1):
            cell = note[2 + half : 3 + half].astype(jnp.int32) + lane
            scale = note[4 + half : 5 + half]
            picks[half, :, at] = jnp.where(cell_at == cell, scale, 0.0).astype(bf16)

    def weigh(first, last):
        @pl.loop(first // 4, last // 4)
        def _(group):
            for i in range(4):
                s = group * 4 + i
                at = pl.ds(pl.multiple_of(s * 128, 128), 128)
                note = told[s]
                tube = jnp.concatenate([note[0:1], note[1:2]], axis=1).astype(jnp.int32)
                select = jnp.where(tube_at == tube, 1.0, 0.0).astype(bf16)
                chosen = lax.dot_general(
                    select,
                    teachers[pl.ds(pl.multiple_of(s * tubes, 16), tubes), :],
                    (((0,), (0,)), ((), ())),
                    preferred_element_type=f32,
                ).astype(bf16)
                rows[0, at, :] = chosen[:128]
                rows[1, at, :] = chosen[128:]

    steps(3, spread)
    steps(2, teach)
    align = gather(own_s, line_s, pairs[3], me.a, 64, ends, twin)
    step(align)

    def add_up(half):
        at = pl.ds(pl.multiple_of(half * 4 * tokens, 128), 4 * tokens)
        parts[at, :] = jnp.dot(picks[half], rows[half], preferred_element_type=f32).astype(bf16)

    half = tokens // 2
    halves = [dict(off=i * half, n=half) for i in (0, 1)]
    weigh(0, 4)
    finish(teach)
    weigh(4, 16)
    merges = [
        reduce(parts, me.row_of, land_0, sums_0, pair, me.b, ends, total, **where)
        for pair, where in zip(pairs[8:10], halves)
    ]
    add_up((me.zh + 1) % 2)
    steps(2, spread)
    steps(2, *merges)
    steps(3, align)
    add_up(me.zh)
    steps(2, align)
    finish(spread)
    steps(2, merges[0])
    steps(4, align)
    steps(2, merges[1])
    finish(*merges)
    target = total[...]
    own_t[...] = (
        target * lax.rsqrt(jnp.sum(target * target, axis=1, keepdims=True) + norm_eps)
    ).astype(bf16)

    moves = [
        (
            gather(own_t, line_t, pairs[4 + 2 * i], me.a, half // 2, ends, twin, **where),
            gather(own_t, column_t, pairs[5 + 2 * i], me.b, half // 2, ends, **where),
        )
        for i, where in enumerate(halves)
    ]
    for move in moves:
        step(*move)
    finish(align)
    wide = 256

    def student(first, last):
        @pl.loop(first, last)
        def _(j):
            at = pl.ds(pl.multiple_of(j * wide, wide), wide)
            gram[:, at] = lax.dot_general(
                column_s[...], line_s[at, :], NT, preferred_element_type=f32
            )

    student(0, 4)
    steps(3, *moves[0])
    student(4, 6)
    steps(3, *moves[1])
    steps(2, *moves[0])
    student(6, 8)
    steps(2, *moves[1])

    def incline(first, last, at_column, columns):
        some = pl.ds(at_column, columns)

        @pl.loop(first, last)
        def _(j):
            at = pl.ds(pl.multiple_of(j * wide, wide), wide)
            gram_t = lax.dot_general(
                column_t[some, :], line_t[at, :], NT, preferred_element_type=f32
            )
            diff = (gram[some, at] - gram_t) * (1.0 / huber_delta)
            slope[some, at] = jnp.clip(diff, -1.0, 1.0).astype(bf16)

    early = 5 * tokens
    incline(0, 2, 0, early)
    finish(*moves[0])
    finish(*moves[1])
    incline(0, 2, early, 8 * tokens - early)
    incline(2, 16 * tokens // wide, 0, 8 * tokens)

    def pull(first, last):
        @pl.loop(first, last)
        def _(i):
            at = pl.ds(pl.multiple_of(i * wide, wide), wide)
            parts[at, :] = jnp.dot(slope[at, :], line_s[...], preferred_element_type=f32).astype(bf16)

    for copy in ends:
        copy.wait_send()
    ends.clear()
    merges = [
        reduce(parts, lambda d, q: q * 4 + d, land_1, sums_1, pair, me.b, ends, total, **where)
        for pair, where in zip(pairs[10:12], halves)
    ]
    pull(3, 4)
    step(*merges)
    pull(2, 3)
    step(*merges)
    pull(0, 2)
    for merge in merges:
        steps(2, merge)
    finish(*merges)
    grad_unit = 2.0 * total[...]
    along = jnp.sum(unit[...] * grad_unit, axis=1, keepdims=True)
    out[...] = ((grad_unit - unit[...] * along) * inverse).astype(bf16)
    for copy in ends:
        copy.wait_send()


def local(student_hidden, projection, teacher, block_map, block_counts, interp_weights):
    (tokens, depth), width = student_hidden.shape, projection.shape[1]
    tubes = teacher.shape[0]
    f32, bf16, i32 = jnp.float32, jnp.bfloat16, jnp.int32
    buffers = (
        ((tokens, depth), bf16),
        ((depth, width), bf16),
        ((3, 32, 128), i32),
        ((16, 8, 128), f32),
        ((tokens, width), f32),
        ((tokens, width), f32),
        ((tokens, width), bf16),
        ((16 * tubes, width), bf16),
        ((16, 8, 128), f32),
        ((2, 2048, width), bf16),
        ((2, 4 * tokens, 2048), bf16),
        ((8 * tokens, width), bf16),
        ((16 * tokens, width), bf16),
        ((8 * tokens, width), bf16),
        ((16 * tokens, width), bf16),
        ((8 * tokens, width), bf16),
        ((tokens, width), bf16),
        ((8 * tokens, 16 * tokens), f32),
        ((8 * tokens, 16 * tokens), bf16),
        ((7 * tokens, width), bf16),
        ((3 * tokens, width), bf16),
        ((7 * tokens, width), bf16),
        ((3 * tokens, width), bf16),
    )
    sems = (17, 16, 9, 17, 17, 9, 17, 9, 10, 10, 10, 10)
    fields = block_map.reshape(3, -1, 128)
    kept = pl.BlockSpec(memory_space=pltpu.VMEM)
    left = pl.BlockSpec(memory_space=pl.ANY)
    grad_proj = pl.pallas_call(
        whole_kernel,
        out_shape=jax.ShapeDtypeStruct((tokens, width), bf16),
        in_specs=[left, left, kept, kept, kept, pl.BlockSpec(memory_space=pltpu.SMEM)],
        out_specs=kept,
        scratch_shapes=[pltpu.VMEM(*b) for b in buffers]
        + [pltpu.SemaphoreType.DMA((2,))]
        + [pltpu.SemaphoreType.DMA((n,)) for n in sems for _ in (0, 1)],
        compiler_params=pltpu.CompilerParams(
            collective_id=1, has_side_effects=True, vmem_limit_bytes=60 * 2**20
        ),
        name="whole_kernel",
    )(student_hidden, projection, teacher, fields, block_counts, interp_weights)
    grad_hidden = lax.dot_general(grad_proj, projection, NT, preferred_element_type=f32)
    return grad_hidden.astype(bf16)


def solution(mesh):
    return jax.shard_map(
        local,
        mesh=mesh,
        in_specs=(
            P(BOTH, None),
            P(),
            P(BOTH, None),
            P(BOTH, None, None),
            P(BOTH, None),
            P(),
        ),
        out_specs=P(BOTH, None),
        check_vma=False,
    )
```

```python
import jax
import jax.numpy as jnp
from jax import lax
from jax.experimental import pallas as pl
from jax.experimental.pallas import tpu as pltpu
from jax.sharding import PartitionSpec as P

BOTH = ("row", "col")
MESH = pl.DeviceIdType.MESH
NT = (((1,), (1,)), ((), ()))

huber_delta = 0.05
norm_eps = 1e-06


class Place:
    def __init__(self):
        row, col = lax.axis_index("row"), lax.axis_index("col")
        self.zh, self.y = row // 4, row % 4
        self.x, self.zl, self.core = col // 4, (col // 2) % 2, col % 2

    def row_of(self, d, q):
        return (self.zh + q) % 2 * 4 + (self.y + d) % 4

    def a(self, d, q, k=0):
        col = (self.x + d) % 4 * 4 + (self.zl + q) % 2 * 2 + (self.core + k) % 2
        return (self.zh * 4 + self.y, col)

    def b(self, d, q):
        col = self.x * 4 + (self.zl + q) % 2 * 2 + self.core
        return (self.row_of(d, q), col)


def greet(peers):
    barrier = pltpu.get_barrier_semaphore()
    for peer in peers:
        pl.semaphore_signal(barrier, inc=1, device_id=peer, device_id_type=MESH)
    pl.semaphore_wait(barrier, len(peers))


def remote(src, dst, send, recv, i, device):
    return pltpu.make_async_remote_copy(
        src_ref=src,
        dst_ref=dst,
        send_sem=send.at[i],
        recv_sem=recv.at[i],
        device_id=device,
        device_id_type=MESH,
    )


def rows_of(ref, at, count):
    return ref.at[pl.ds(pl.multiple_of(at, 16), count)]


def gather(own, buf, sems, to, cut, ends, twin=None, off=0, n=None):
    send, recv = sems
    size = own.shape[0]
    n = n or size
    own = rows_of(own, off, n)

    def part(block, start=0, count=n):
        return rows_of(buf, block * size + off + start, count)

    ahead, behind, across = to(1, 0), to(3, 0), to(0, 1)
    lo, hi = (0, cut), (cut, n - cut)
    plan = [
        (own, part(3), ahead),
        (own, part(1), behind),
        (own, part(4), across),
        (part(3, *lo), part(2, *lo), ahead),
        (part(1, *hi), part(2, *hi), behind),
        (part(4), part(7), ahead),
        (part(4), part(5), behind),
        (part(2, *lo), part(6, *lo), across),
        (part(2, *hi), part(6, *hi), across),
    ]
    copies = [remote(s, d, send, recv, i, dev) for i, (s, d, dev) in enumerate(plan)]
    ends.extend(copies)
    twins = []

    def pass_on(src, block):
        if twin is not None:
            copy = remote(src, part(8 + block), send, recv, 9 + block, twin)
            copy.start()
            twins.append(copy)
            ends.append(copy)

    for i in (0, 1, 2):
        copies[i].start()
    pass_on(own, 0)
    buf[off : off + n, :] = own[...]
    yield
    after = ((0, (3,), 3), (1, (4,), 1), (2, (5, 6), 4), (3, (7,), None), (4, (8,), 2))
    after += ((5, (), 7), (6, (), 5), (7, (), None), (8, (), 6))
    for i, starts, block in after:
        copies[i].wait_recv()
        for j in starts:
            copies[j].start()
        if block is not None:
            pass_on(part(block), block)
        yield
    for copy in twins:
        copy.wait_recv()


def reduce(blocks, block_of, land, sums, sems, to, ends, total, off=0, n=None):
    send, recv = sems
    size = total.shape[0]
    n = n or size
    half = n // 2
    ahead, behind, across = to(1, 0), to(3, 0), to(0, 1)

    def mine(d, q, start=0, count=n):
        return rows_of(blocks, block_of(d, q) * size + off + start, count)

    def at(ref, slot, start=0, count=n):
        return rows_of(ref, slot * size + off + start, count)

    def wide(ref):
        return ref[...].astype(jnp.float32)

    lo, hi = (0, half), (half, half)
    plan = [
        (mine(2, 1), at(land, 0), across),
        (mine(1, 1), at(land, 1), ahead),
        (mine(3, 1), at(land, 2), behind),
        (at(sums, 0, *lo), at(land, 3, *lo), ahead),
        (at(sums, 0, *hi), at(land, 3, *hi), behind),
        (at(sums, 1), at(land, 4), across),
        (mine(1, 0, *hi), at(land, 5, *hi), ahead),
        (at(sums, 2, *lo), at(land, 5, *lo), ahead),
        (mine(3, 0, *lo), at(land, 6, *lo), behind),
        (at(sums, 2, *hi), at(land, 6, *hi), behind),
    ]
    copies = [remote(s, d, send, recv, i, dev) for i, (s, d, dev) in enumerate(plan)]
    ends.extend(copies)

    def store(slot, start, count, *terms):
        value = wide(terms[0])
        for term in terms[1:]:
            value = value + wide(term)
        at(sums, slot, start, count)[...] = value.astype(jnp.bfloat16)

    copies[0].start()
    copies[2].start()
    yield
    copies[1].start()
    yield
    copies[0].wait_recv()
    store(0, 0, n, mine(2, 0), at(land, 0))
    copies[3].start()
    copies[4].start()
    copies[6].start()
    copies[8].start()
    yield
    copies[1].wait_recv()
    copies[2].wait_recv()
    store(1, 0, n, mine(0, 1), at(land, 1), at(land, 2))
    copies[5].start()
    yield
    copies[3].wait_recv()
    store(2, *lo, mine(1, 0, *lo), at(land, 3, *lo))
    copies[7].start()
    copies[4].wait_recv()
    store(2, *hi, mine(3, 0, *hi), at(land, 3, *hi))
    copies[9].start()
    yield
    for i in (6, 8, 5, 7, 9):
        copies[i].wait_recv()
    landed = wide(at(land, 4)) + wide(at(land, 5)) + wide(at(land, 6))
    total[off : off + n, :] = wide(mine(0, 0)) + landed


def step(*plans):
    for plan in plans:
        next(plan, None)


def steps(count, *plans):
    for _ in range(count):
        step(*plans)


def finish(*plans):
    plans = list(plans)
    while plans:
        for plan in list(plans):
            try:
                next(plan)
            except StopIteration:
                plans.remove(plan)


def write_notes(block_map, block_counts, interp_weights, before, notes):
    f32, i32 = jnp.float32, jnp.int32
    for y in range(4):
        for x in range(4):
            for zh in (0, 1):
                chunk = (zh * 4 + y) * 4 + x
                row = y * 8 + x * 2 + zh
                for field in range(3):
                    before[field, row : row + 1, :] = block_map[field, chunk : chunk + 1, :]
    row = lax.broadcasted_iota(i32, (32, 128), 0)
    column = lax.broadcasted_iota(i32, (32, 128), 1)
    chunk = (row % 2 * 4 + row // 8) * 4 + row % 8 // 2
    counts = jnp.where(column // 4 == chunk, block_counts[...], 0).astype(f32).astype(jnp.bfloat16)
    source = lax.broadcasted_iota(i32, (128, 128), 0)
    lane = lax.broadcasted_iota(i32, (128, 128), 1)
    spread = jnp.where(source % 4 == lane // 32, 1.0, 0.0).astype(jnp.bfloat16)
    counts = jnp.dot(counts, spread, preferred_element_type=f32).astype(i32)
    level = before[2]
    scale = jnp.zeros((32, 128), f32)
    for l in range(interp_weights.shape[0]):
        scale = jnp.where(level == l, interp_weights[l], scale)
    scale = jnp.where(column % 32 < counts, scale, 0.0)
    notes[...] = jnp.zeros_like(notes)
    for field, value in enumerate((before[0].astype(f32), before[1].astype(f32), scale)):
        for g in range(4):
            pieces = [value[y * 8 : y * 8 + 8, g * 32 : g * 32 + 32] for y in range(4)]
            turned = jnp.concatenate(pieces, axis=1)
            for x in range(4):
                for zh in (0, 1):
                    note = x * 4 + (g // 2 + zh) % 2 * 2 + g % 2
                    at = field * 2 + zh
                    notes[note, at : at + 1, :] = turned[x * 2 + zh : x * 2 + zh + 1]


def whole_kernel(
    hidden_in, projection_in, teacher, block_map, block_counts, interp_weights, out,
    hidden, projection, before, notes, unit, total, own_s,
    teachers, told, rows, picks, parts, line_s, column_s, line_t, column_t, own_t, gram, slope,
    land_0, sums_0, land_1, sums_1, loads, *sems,
):
    f32, bf16 = jnp.float32, jnp.bfloat16
    pairs = [sems[i : i + 2] for i in range(0, len(sems), 2)]
    me = Place()
    twin = me.a(0, 0, 1)
    tubes, tokens = teacher.shape[0], own_s.shape[0]
    load_hidden = pltpu.make_async_copy(hidden_in, hidden, loads.at[0])
    load_projection = pltpu.make_async_copy(projection_in, projection, loads.at[1])
    load_hidden.start()
    load_projection.start()
    others = [(d, q, k) for k in (0, 1) for q in (0, 1) for d in range(4) if d or q or k]
    greet([me.a(*o) for o in others] + [me.b(1, 0), me.b(3, 0), me.b(0, 1)])
    ends = []

    teach = gather(teacher, teachers, pairs[0], me.a, 48, ends, twin)
    step(teach)
    write_notes(block_map, block_counts, interp_weights, before, notes)
    told_by = []
    for d, q, k in others:
        twist = (me.zh + me.zl + q) % 2
        note = (me.x + d) % 4 * 4 + twist * 2 + (me.core + k) % 2
        slot = k * 8 + q * 4 + (4 - d) % 4
        copy = remote(notes.at[note], told.at[slot], *pairs[1], slot, me.a(d, q, k))
        copy.start()
        told_by.append(copy)
        ends.append(copy)
    told[0] = notes[me.x * 4 + (me.zh + me.zl) % 2 * 2 + me.core]
    load_hidden.wait()
    load_projection.wait()
    proj = jnp.dot(hidden[...], projection[...], preferred_element_type=f32)
    inverse = lax.rsqrt(jnp.sum(proj * proj, axis=1, keepdims=True) + norm_eps)
    unit[...] = proj * inverse
    own_s[...] = (proj * inverse).astype(bf16)
    spread = gather(own_s, column_s, pairs[2], me.b, 64, ends)
    step(spread)
    steps(3, teach)
    for copy in told_by:
        copy.wait_recv()

    lane = lax.broadcasted_iota(jnp.int32, (1, 128), 1) // 32 * 128
    tube_at = lax.broadcasted_iota(jnp.int32, (tubes, 256), 0)
    cell_at = lax.broadcasted_iota(jnp.int32, (4 * tokens, 128), 0)

    @pl.loop(0, 16)
    def _(s):
        at = pl.ds(pl.multiple_of(s * 128, 128), 128)
        note = told[s]
        for half in (0, 1):
            cell = note[2 + half : 3 + half].astype(jnp.int32) + lane
            scale = note[4 + half : 5 + half]
            picks[half, :, at] = jnp.where(cell_at == cell, scale, 0.0).astype(bf16)

    def weigh(first, last):
        @pl.loop(first // 4, last // 4)
        def _(group):
            for i in range(4):
                s = group * 4 + i
                at = pl.ds(pl.multiple_of(s * 128, 128), 128)
                note = told[s]
                tube = jnp.concatenate([note[0:1], note[1:2]], axis=1).astype(jnp.int32)
                select = jnp.where(tube_at == tube, 1.0, 0.0).astype(bf16)
                chosen = lax.dot_general(
                    select,
                    teachers[pl.ds(pl.multiple_of(s * tubes, 16), tubes), :],
                    (((0,), (0,)), ((), ())),
                    preferred_element_type=f32,
                ).astype(bf16)
                rows[0, at, :] = chosen[:128]
                rows[1, at, :] = chosen[128:]

    steps(2, teach)
    align = gather(own_s, line_s, pairs[3], me.a, 64, ends, twin)
    step(align)
    steps(3, spread)

    def add_up(half):
        at = pl.ds(pl.multiple_of(half * 4 * tokens, 128), 4 * tokens)
        parts[at, :] = jnp.dot(picks[half], rows[half], preferred_element_type=f32).astype(bf16)

    half = tokens // 2
    halves = [dict(off=i * half, n=half) for i in (0, 1)]
    finish(teach)
    weigh(0, 16)
    steps(2, spread)
    merges = [
        reduce(parts, me.row_of, land_0, sums_0, pair, me.b, ends, total, **where)
        for pair, where in zip(pairs[8:10], halves)
    ]
    add_up((me.zh + 1) % 2)
    steps(2, *merges)
    steps(3, align)
    add_up(me.zh)
    steps(2, align)
    steps(2, merges[0])
    steps(2, merges[1])
    steps(4, align)
    finish(spread)
    finish(*merges)
    target = total[...]
    own_t[...] = (
        target * lax.rsqrt(jnp.sum(target * target, axis=1, keepdims=True) + norm_eps)
    ).astype(bf16)

    moves = [
        (
            gather(own_t, line_t, pairs[4 + 2 * i], me.a, half // 2, ends, twin, **where),
            gather(own_t, column_t, pairs[5 + 2 * i], me.b, half // 2, ends, **where),
        )
        for i, where in enumerate(halves)
    ]
    for move in moves:
        step(*move)
    finish(align)
    wide = 256

    def student(first, last):
        @pl.loop(first, last)
        def _(j):
            at = pl.ds(pl.multiple_of(j * wide, wide), wide)
            gram[:, at] = lax.dot_general(
                column_s[...], line_s[at, :], NT, preferred_element_type=f32
            )

    student(0, 4)
    steps(3, *moves[0])
    student(4, 6)
    steps(3, *moves[1])
    steps(2, *moves[0])
    student(6, 8)
    steps(2, *moves[1])

    def incline(first, last, at_column, columns):
        some = pl.ds(at_column, columns)

        @pl.loop(first, last)
        def _(j):
            at = pl.ds(pl.multiple_of(j * wide, wide), wide)
            gram_t = lax.dot_general(
                column_t[some, :], line_t[at, :], NT, preferred_element_type=f32
            )
            diff = (gram[some, at] - gram_t) * (1.0 / huber_delta)
            slope[some, at] = jnp.clip(diff, -1.0, 1.0).astype(bf16)

    early = 5 * tokens
    incline(0, 2, 0, early)
    finish(*moves[0])
    finish(*moves[1])
    incline(0, 2, early, 8 * tokens - early)
    incline(2, 16 * tokens // wide, 0, 8 * tokens)

    def pull(first, last):
        @pl.loop(first, last)
        def _(i):
            at = pl.ds(pl.multiple_of(i * wide, wide), wide)
            parts[at, :] = jnp.dot(slope[at, :], line_s[...], preferred_element_type=f32).astype(bf16)

    for copy in ends:
        copy.wait_send()
    ends.clear()
    merges = [
        reduce(parts, lambda d, q: q * 4 + d, land_1, sums_1, pair, me.b, ends, total, **where)
        for pair, where in zip(pairs[10:12], halves)
    ]
    pull(3, 4)
    step(*merges)
    pull(2, 3)
    step(*merges)
    pull(0, 2)
    for merge in merges:
        steps(2, merge)
    finish(*merges)
    grad_unit = 2.0 * total[...]
    along = jnp.sum(unit[...] * grad_unit, axis=1, keepdims=True)
    out[...] = ((grad_unit - unit[...] * along) * inverse).astype(bf16)
    for copy in ends:
        copy.wait_send()


def local(student_hidden, projection, teacher, block_map, block_counts, interp_weights):
    (tokens, depth), width = student_hidden.shape, projection.shape[1]
    tubes = teacher.shape[0]
    f32, bf16, i32 = jnp.float32, jnp.bfloat16, jnp.int32
    buffers = (
        ((tokens, depth), bf16),
        ((depth, width), bf16),
        ((3, 32, 128), i32),
        ((16, 8, 128), f32),
        ((tokens, width), f32),
        ((tokens, width), f32),
        ((tokens, width), bf16),
        ((16 * tubes, width), bf16),
        ((16, 8, 128), f32),
        ((2, 2048, width), bf16),
        ((2, 4 * tokens, 2048), bf16),
        ((8 * tokens, width), bf16),
        ((16 * tokens, width), bf16),
        ((8 * tokens, width), bf16),
        ((16 * tokens, width), bf16),
        ((8 * tokens, width), bf16),
        ((tokens, width), bf16),
        ((8 * tokens, 16 * tokens), f32),
        ((8 * tokens, 16 * tokens), bf16),
        ((7 * tokens, width), bf16),
        ((3 * tokens, width), bf16),
        ((7 * tokens, width), bf16),
        ((3 * tokens, width), bf16),
    )
    sems = (17, 16, 9, 17, 17, 9, 17, 9, 10, 10, 10, 10)
    fields = block_map.reshape(3, -1, 128)
    kept = pl.BlockSpec(memory_space=pltpu.VMEM)
    left = pl.BlockSpec(memory_space=pl.ANY)
    grad_proj = pl.pallas_call(
        whole_kernel,
        out_shape=jax.ShapeDtypeStruct((tokens, width), bf16),
        in_specs=[left, left, kept, kept, kept, pl.BlockSpec(memory_space=pltpu.SMEM)],
        out_specs=kept,
        scratch_shapes=[pltpu.VMEM(*b) for b in buffers]
        + [pltpu.SemaphoreType.DMA((2,))]
        + [pltpu.SemaphoreType.DMA((n,)) for n in sems for _ in (0, 1)],
        compiler_params=pltpu.CompilerParams(
            collective_id=1, has_side_effects=True, vmem_limit_bytes=60 * 2**20
        ),
        name="whole_kernel",
    )(student_hidden, projection, teacher, fields, block_counts, interp_weights)
    grad_hidden = lax.dot_general(grad_proj, projection, NT, preferred_element_type=f32)
    return grad_hidden.astype(bf16)


def solution(mesh):
    return jax.shard_map(
        local,
        mesh=mesh,
        in_specs=(
            P(BOTH, None),
            P(),
            P(BOTH, None),
            P(BOTH, None, None),
            P(BOTH, None),
            P(),
        ),
        out_specs=P(BOTH, None),
        check_vma=False,
    )
```

```python
import jax
import jax.numpy as jnp
from jax import lax
from jax.experimental import pallas as pl
from jax.experimental.pallas import tpu as pltpu
from jax.sharding import PartitionSpec as P

BOTH = ("row", "col")
MESH = pl.DeviceIdType.MESH
NT = (((1,), (1,)), ((), ()))

huber_delta = 0.05
norm_eps = 1e-06


class Place:
    def __init__(self):
        row, col = lax.axis_index("row"), lax.axis_index("col")
        self.zh, self.y = row // 4, row % 4
        self.x, self.zl, self.core = col // 4, (col // 2) % 2, col % 2

    def row_of(self, d, q):
        return (self.zh + q) % 2 * 4 + (self.y + d) % 4

    def a(self, d, q, k=0):
        col = (self.x + d) % 4 * 4 + (self.zl + q) % 2 * 2 + (self.core + k) % 2
        return (self.zh * 4 + self.y, col)

    def b(self, d, q):
        col = self.x * 4 + (self.zl + q) % 2 * 2 + self.core
        return (self.row_of(d, q), col)


def greet(peers):
    barrier = pltpu.get_barrier_semaphore()
    for peer in peers:
        pl.semaphore_signal(barrier, inc=1, device_id=peer, device_id_type=MESH)
    pl.semaphore_wait(barrier, len(peers))


def remote(src, dst, send, recv, i, device):
    return pltpu.make_async_remote_copy(
        src_ref=src,
        dst_ref=dst,
        send_sem=send.at[i],
        recv_sem=recv.at[i],
        device_id=device,
        device_id_type=MESH,
    )


def rows_of(ref, at, count):
    return ref.at[pl.ds(pl.multiple_of(at, 16), count)]


def gather(own, buf, sems, to, cut, ends, twin=None, off=0, n=None):
    send, recv = sems
    size = own.shape[0]
    n = n or size
    own = rows_of(own, off, n)

    def part(block, start=0, count=n):
        return rows_of(buf, block * size + off + start, count)

    ahead, behind, across = to(1, 0), to(3, 0), to(0, 1)
    lo, hi = (0, cut), (cut, n - cut)
    plan = [
        (own, part(3), ahead),
        (own, part(1), behind),
        (own, part(4), across),
        (part(3, *lo), part(2, *lo), ahead),
        (part(1, *hi), part(2, *hi), behind),
        (part(4), part(7), ahead),
        (part(4), part(5), behind),
        (part(2, *lo), part(6, *lo), across),
        (part(2, *hi), part(6, *hi), across),
    ]
    copies = [remote(s, d, send, recv, i, dev) for i, (s, d, dev) in enumerate(plan)]
    ends.extend(copies)
    twins = []

    def pass_on(src, block):
        if twin is not None:
            copy = remote(src, part(8 + block), send, recv, 9 + block, twin)
            copy.start()
            twins.append(copy)
            ends.append(copy)

    for i in (0, 1, 2):
        copies[i].start()
    pass_on(own, 0)
    buf[off : off + n, :] = own[...]
    yield
    after = ((0, (3,), 3), (1, (4,), 1), (2, (5, 6), 4), (3, (7,), None), (4, (8,), 2))
    after += ((5, (), 7), (6, (), 5), (7, (), None), (8, (), 6))
    for i, starts, block in after:
        copies[i].wait_recv()
        for j in starts:
            copies[j].start()
        if block is not None:
            pass_on(part(block), block)
        yield
    for copy in twins:
        copy.wait_recv()


def reduce(blocks, block_of, land, sums, sems, to, ends, total, off=0, n=None):
    send, recv = sems
    size = total.shape[0]
    n = n or size
    half = n // 2
    ahead, behind, across = to(1, 0), to(3, 0), to(0, 1)

    def mine(d, q, start=0, count=n):
        return rows_of(blocks, block_of(d, q) * size + off + start, count)

    def at(ref, slot, start=0, count=n):
        return rows_of(ref, slot * size + off + start, count)

    def wide(ref):
        return ref[...].astype(jnp.float32)

    lo, hi = (0, half), (half, half)
    plan = [
        (mine(2, 1), at(land, 0), across),
        (mine(1, 1), at(land, 1), ahead),
        (mine(3, 1), at(land, 2), behind),
        (at(sums, 0, *lo), at(land, 3, *lo), ahead),
        (at(sums, 0, *hi), at(land, 3, *hi), behind),
        (at(sums, 1), at(land, 4), across),
        (mine(1, 0, *hi), at(land, 5, *hi), ahead),
        (at(sums, 2, *lo), at(land, 5, *lo), ahead),
        (mine(3, 0, *lo), at(land, 6, *lo), behind),
        (at(sums, 2, *hi), at(land, 6, *hi), behind),
    ]
    copies = [remote(s, d, send, recv, i, dev) for i, (s, d, dev) in enumerate(plan)]
    ends.extend(copies)

    def store(slot, start, count, *terms):
        value = wide(terms[0])
        for term in terms[1:]:
            value = value + wide(term)
        at(sums, slot, start, count)[...] = value.astype(jnp.bfloat16)

    copies[0].start()
    copies[2].start()
    yield
    copies[1].start()
    yield
    copies[0].wait_recv()
    store(0, 0, n, mine(2, 0), at(land, 0))
    copies[3].start()
    copies[4].start()
    copies[6].start()
    copies[8].start()
    yield
    copies[1].wait_recv()
    copies[2].wait_recv()
    store(1, 0, n, mine(0, 1), at(land, 1), at(land, 2))
    copies[5].start()
    yield
    copies[3].wait_recv()
    store(2, *lo, mine(1, 0, *lo), at(land, 3, *lo))
    copies[7].start()
    copies[4].wait_recv()
    store(2, *hi, mine(3, 0, *hi), at(land, 3, *hi))
    copies[9].start()
    yield
    for i in (6, 8, 5, 7, 9):
        copies[i].wait_recv()
    landed = wide(at(land, 4)) + wide(at(land, 5)) + wide(at(land, 6))
    total[off : off + n, :] = wide(mine(0, 0)) + landed


def step(*plans):
    for plan in plans:
        next(plan, None)


def steps(count, *plans):
    for _ in range(count):
        step(*plans)


def finish(*plans):
    plans = list(plans)
    while plans:
        for plan in list(plans):
            try:
                next(plan)
            except StopIteration:
                plans.remove(plan)


def write_notes(block_map, block_counts, interp_weights, before, notes):
    f32, i32 = jnp.float32, jnp.int32
    for y in range(4):
        for x in range(4):
            for zh in (0, 1):
                chunk = (zh * 4 + y) * 4 + x
                row = y * 8 + x * 2 + zh
                for field in range(3):
                    before[field, row : row + 1, :] = block_map[field, chunk : chunk + 1, :]
    row = lax.broadcasted_iota(i32, (32, 128), 0)
    column = lax.broadcasted_iota(i32, (32, 128), 1)
    chunk = (row % 2 * 4 + row // 8) * 4 + row % 8 // 2
    counts = jnp.where(column // 4 == chunk, block_counts[...], 0).astype(f32).astype(jnp.bfloat16)
    source = lax.broadcasted_iota(i32, (128, 128), 0)
    lane = lax.broadcasted_iota(i32, (128, 128), 1)
    spread = jnp.where(source % 4 == lane // 32, 1.0, 0.0).astype(jnp.bfloat16)
    counts = jnp.dot(counts, spread, preferred_element_type=f32).astype(i32)
    level = before[2]
    scale = jnp.zeros((32, 128), f32)
    for l in range(interp_weights.shape[0]):
        scale = jnp.where(level == l, interp_weights[l], scale)
    scale = jnp.where(column % 32 < counts, scale, 0.0)
    notes[...] = jnp.zeros_like(notes)
    for field, value in enumerate((before[0].astype(f32), before[1].astype(f32), scale)):
        for g in range(4):
            pieces = [value[y * 8 : y * 8 + 8, g * 32 : g * 32 + 32] for y in range(4)]
            turned = jnp.concatenate(pieces, axis=1)
            for x in range(4):
                for zh in (0, 1):
                    note = x * 4 + (g // 2 + zh) % 2 * 2 + g % 2
                    at = field * 2 + zh
                    notes[note, at : at + 1, :] = turned[x * 2 + zh : x * 2 + zh + 1]


def whole_kernel(
    hidden_in, projection_in, teacher, block_map, block_counts, interp_weights, out,
    hidden, projection, before, notes, unit, total, own_s,
    teachers, told, rows, picks, parts, line_s, column_s, line_t, column_t, own_t, gram, slope,
    land_0, sums_0, land_1, sums_1, loads, *sems,
):
    f32, bf16 = jnp.float32, jnp.bfloat16
    pairs = [sems[i : i + 2] for i in range(0, len(sems), 2)]
    me = Place()
    twin = me.a(0, 0, 1)
    tubes, tokens = teacher.shape[0], own_s.shape[0]
    load_hidden = pltpu.make_async_copy(hidden_in, hidden, loads.at[0])
    load_projection = pltpu.make_async_copy(projection_in, projection, loads.at[1])
    load_hidden.start()
    load_projection.start()
    others = [(d, q, k) for k in (0, 1) for q in (0, 1) for d in range(4) if d or q or k]
    greet([me.a(*o) for o in others] + [me.b(1, 0), me.b(3, 0), me.b(0, 1)])
    ends = []

    teach = gather(teacher, teachers, pairs[0], me.a, 48, ends, twin)
    step(teach)
    write_notes(block_map, block_counts, interp_weights, before, notes)
    told_by = []
    for d, q, k in others:
        twist = (me.zh + me.zl + q) % 2
        note = (me.x + d) % 4 * 4 + twist * 2 + (me.core + k) % 2
        slot = k * 8 + q * 4 + (4 - d) % 4
        copy = remote(notes.at[note], told.at[slot], *pairs[1], slot, me.a(d, q, k))
        copy.start()
        told_by.append(copy)
        ends.append(copy)
    told[0] = notes[me.x * 4 + (me.zh + me.zl) % 2 * 2 + me.core]
    load_hidden.wait()
    load_projection.wait()
    proj = jnp.dot(hidden[...], projection[...], preferred_element_type=f32)
    inverse = lax.rsqrt(jnp.sum(proj * proj, axis=1, keepdims=True) + norm_eps)
    unit[...] = proj * inverse
    own_s[...] = (proj * inverse).astype(bf16)
    spread = gather(own_s, column_s, pairs[2], me.b, 64, ends)
    step(spread)
    steps(3, teach)
    for copy in told_by:
        copy.wait_recv()

    lane = lax.broadcasted_iota(jnp.int32, (1, 128), 1) // 32 * 128
    tube_at = lax.broadcasted_iota(jnp.int32, (tubes, 256), 0)
    cell_at = lax.broadcasted_iota(jnp.int32, (4 * tokens, 128), 0)

    @pl.loop(0, 16)
    def _(s):
        at = pl.ds(pl.multiple_of(s * 128, 128), 128)
        note = told[s]
        for half in (0, 1):
            cell = note[2 + half : 3 + half].astype(jnp.int32) + lane
            scale = note[4 + half : 5 + half]
            picks[half, :, at] = jnp.where(cell_at == cell, scale, 0.0).astype(bf16)

    def weigh(first, last):
        @pl.loop(first // 4, last // 4)
        def _(group):
            for i in range(4):
                s = group * 4 + i
                at = pl.ds(pl.multiple_of(s * 128, 128), 128)
                note = told[s]
                tube = jnp.concatenate([note[0:1], note[1:2]], axis=1).astype(jnp.int32)
                select = jnp.where(tube_at == tube, 1.0, 0.0).astype(bf16)
                chosen = lax.dot_general(
                    select,
                    teachers[pl.ds(pl.multiple_of(s * tubes, 16), tubes), :],
                    (((0,), (0,)), ((), ())),
                    preferred_element_type=f32,
                ).astype(bf16)
                rows[0, at, :] = chosen[:128]
                rows[1, at, :] = chosen[128:]

    steps(2, teach)
    align = gather(own_s, line_s, pairs[3], me.a, 64, ends, twin)
    step(align)
    steps(3, spread)

    def add_up(half):
        at = pl.ds(pl.multiple_of(half * 4 * tokens, 128), 4 * tokens)
        parts[at, :] = jnp.dot(picks[half], rows[half], preferred_element_type=f32).astype(bf16)

    half = tokens // 2
    halves = [dict(off=i * half, n=half) for i in (0, 1)]
    finish(teach)
    weigh(0, 16)
    steps(2, spread)
    merges = [
        reduce(parts, me.row_of, land_0, sums_0, pair, me.b, ends, total, **where)
        for pair, where in zip(pairs[8:10], halves)
    ]
    add_up((me.zh + 1) % 2)
    steps(2, *merges)
    steps(3, align)
    add_up(me.zh)
    steps(2, align)
    steps(2, merges[0])
    steps(2, merges[1])
    steps(4, align)
    finish(spread)
    finish(*merges)
    target = total[...]
    own_t[...] = (
        target * lax.rsqrt(jnp.sum(target * target, axis=1, keepdims=True) + norm_eps)
    ).astype(bf16)

    moves = [
        (
            gather(own_t, line_t, pairs[4 + 2 * i], me.a, half // 2, ends, twin, **where),
            gather(own_t, column_t, pairs[5 + 2 * i], me.b, half // 2, ends, **where),
        )
        for i, where in enumerate(halves)
    ]
    for move in moves:
        step(*move)
    finish(align)
    wide = 256

    def student(first, last):
        @pl.loop(first, last)
        def _(j):
            at = pl.ds(pl.multiple_of(j * wide, wide), wide)
            gram[:, at] = lax.dot_general(
                column_s[...], line_s[at, :], NT, preferred_element_type=f32
            )

    student(0, 6)
    steps(3, *moves[0])
    steps(3, *moves[1])
    student(6, 8)
    steps(2, *moves[0])
    steps(2, *moves[1])

    def incline(first, last, at_column, columns):
        some = pl.ds(at_column, columns)

        @pl.loop(first, last)
        def _(j):
            at = pl.ds(pl.multiple_of(j * wide, wide), wide)
            gram_t = lax.dot_general(
                column_t[some, :], line_t[at, :], NT, preferred_element_type=f32
            )
            diff = (gram[some, at] - gram_t) * (1.0 / huber_delta)
            slope[some, at] = jnp.clip(diff, -1.0, 1.0).astype(bf16)

    early = 5 * tokens
    incline(0, 2, 0, early)
    finish(*moves[0])
    finish(*moves[1])
    incline(0, 2, early, 8 * tokens - early)
    incline(2, 16 * tokens // wide, 0, 8 * tokens)

    def pull(first, last):
        @pl.loop(first, last)
        def _(i):
            at = pl.ds(pl.multiple_of(i * wide, wide), wide)
            parts[at, :] = jnp.dot(slope[at, :], line_s[...], preferred_element_type=f32).astype(bf16)

    for copy in ends:
        copy.wait_send()
    ends.clear()
    merges = [
        reduce(parts, lambda d, q: q * 4 + d, land_1, sums_1, pair, me.b, ends, total, **where)
        for pair, where in zip(pairs[10:12], halves)
    ]
    pull(3, 4)
    step(*merges)
    pull(2, 3)
    step(*merges)
    pull(0, 2)
    for merge in merges:
        steps(2, merge)
    finish(*merges)
    grad_unit = 2.0 * total[...]
    along = jnp.sum(unit[...] * grad_unit, axis=1, keepdims=True)
    out[...] = ((grad_unit - unit[...] * along) * inverse).astype(bf16)
    for copy in ends:
        copy.wait_send()


def local(student_hidden, projection, teacher, block_map, block_counts, interp_weights):
    (tokens, depth), width = student_hidden.shape, projection.shape[1]
    tubes = teacher.shape[0]
    f32, bf16, i32 = jnp.float32, jnp.bfloat16, jnp.int32
    buffers = (
        ((tokens, depth), bf16),
        ((depth, width), bf16),
        ((3, 32, 128), i32),
        ((16, 8, 128), f32),
        ((tokens, width), f32),
        ((tokens, width), f32),
        ((tokens, width), bf16),
        ((16 * tubes, width), bf16),
        ((16, 8, 128), f32),
        ((2, 2048, width), bf16),
        ((2, 4 * tokens, 2048), bf16),
        ((8 * tokens, width), bf16),
        ((16 * tokens, width), bf16),
        ((8 * tokens, width), bf16),
        ((16 * tokens, width), bf16),
        ((8 * tokens, width), bf16),
        ((tokens, width), bf16),
        ((8 * tokens, 16 * tokens), f32),
        ((8 * tokens, 16 * tokens), bf16),
        ((7 * tokens, width), bf16),
        ((3 * tokens, width), bf16),
        ((7 * tokens, width), bf16),
        ((3 * tokens, width), bf16),
    )
    sems = (17, 16, 9, 17, 17, 9, 17, 9, 10, 10, 10, 10)
    fields = block_map.reshape(3, -1, 128)
    kept = pl.BlockSpec(memory_space=pltpu.VMEM)
    left = pl.BlockSpec(memory_space=pl.ANY)
    grad_proj = pl.pallas_call(
        whole_kernel,
        out_shape=jax.ShapeDtypeStruct((tokens, width), bf16),
        in_specs=[left, left, kept, kept, kept, pl.BlockSpec(memory_space=pltpu.SMEM)],
        out_specs=kept,
        scratch_shapes=[pltpu.VMEM(*b) for b in buffers]
        + [pltpu.SemaphoreType.DMA((2,))]
        + [pltpu.SemaphoreType.DMA((n,)) for n in sems for _ in (0, 1)],
        compiler_params=pltpu.CompilerParams(
            collective_id=1, has_side_effects=True, vmem_limit_bytes=60 * 2**20
        ),
        name="whole_kernel",
    )(student_hidden, projection, teacher, fields, block_counts, interp_weights)
    grad_hidden = lax.dot_general(grad_proj, projection, NT, preferred_element_type=f32)
    return grad_hidden.astype(bf16)


def solution(mesh):
    return jax.shard_map(
        local,
        mesh=mesh,
        in_specs=(
            P(BOTH, None),
            P(),
            P(BOTH, None),
            P(BOTH, None, None),
            P(BOTH, None),
            P(),
        ),
        out_specs=P(BOTH, None),
        check_vma=False,
    )
```
